128 devices in a mesh: tm: 64 (over z, y, x_lo, core), space: 2 (over x_hi).
Axes of the slice: x: 4 (x_hi: 2, x_lo: 2; x = x_hi * 2 + x_lo), y: 4, z: 4, core: 2. Of those that a mesh axis runs over, the one named last changes fastest.
Arguments:
- u_init: float32 [2, 512, 512], P(None, 'space'), may hold values from -8 to 8
- phase: float32 [512, 512], P('space'), may hold values from 0.005 to 0.05
- absorb: float32 [512, 512], P('space'), may hold values from 0.004 to 0.04
Outputs:
- solution: float32 [2, 64, 512, 512], P(None, 'tm', 'space')
The draws below stay inside these ranges and needn't reach their ends.
All inputs are finite; a program needn't handle non-finite values.
Results may differ from the reference program's by a relative error of at most 0.0003.
Values sent between devices are 32-bit elements; how exact they have to be, the bound alone decides.
No kernel may reach another device: no remote copies, remote signals or barrier semaphores. Data moves between devices by JAX's collectives and lax.ppermute only.
A program may use at most 192 MiB of HBM per device.

```python
import math
import jax
import jax.numpy as jnp

NX = 512
NY = 512
ITERS = 4
TIME = 64


def draw_u_init(key, part):
    key_noise = jax.random.fold_in(key, 11)
    noise = jax.random.normal(key_noise, (2, NX, NY), jnp.float32)
    return jnp.clip(noise, -6.0, 6.0)


def block_levels(stream_key, dims, pieces, smallest, top_value):
    factor_of, own = 1.0, jax.random.fold_in(stream_key, 6)
    for axis_at, shards_of in pieces:
        draws = jnp.exp(jax.random.uniform(jax.random.fold_in(own, axis_at), (shards_of,), jnp.float32, smallest / len(pieces), top_value / len(pieces)))
        factor_of = factor_of * jnp.repeat(draws, dims[axis_at] // shards_of).reshape([-1 if axis == axis_at else 1 for axis in range(len(dims))])
    return factor_of


def setup_inputs(seed: int = 0) -> dict:
    arg_keys = jax.random.split(jax.random.key(seed), 4)
    return {
        "u_init": draw_u_init(jax.random.fold_in(arg_keys[3], 71), 0),
        "phase": jnp.clip(jnp.exp(math.log(0.05) - 2.3025851 * jax.random.uniform(arg_keys[1], (NX, NY), jnp.float32) ** block_levels(arg_keys[1], (NX, NY), ((0, 2),), -0.2, 0.2)), 0.005, 0.05),
        "absorb": jnp.clip(jnp.exp(math.log(0.04) - 2.30258502 * jax.random.uniform(arg_keys[2], (NX, NY), jnp.float32) ** block_levels(arg_keys[2], (NX, NY), ((0, 2),), -0.2, 0.2)), 0.004, 0.04),
    }


tau = 400.0
alpha = 0.4

def laplacian(field):
    return jnp.roll(field, 1, -2) + jnp.roll(field, -1, -2) + jnp.roll(field, 1, -1) + jnp.roll(field, -1, -1) - 4.0 * field

def generator(field, phase, absorb):
    curvature = laplacian(field)
    change_real = -tau * curvature[1] + phase * field[1] - absorb * field[0]
    change_imag = tau * curvature[0] - phase * field[0] - absorb * field[1]
    return jnp.stack([change_real, change_imag])

def operate(field, phase, absorb):
    change = generator(field, phase, absorb)
    ahead = field + 0.5 * change
    behind = field - 0.5 * change
    previous = jnp.concatenate([jnp.zeros_like(ahead[:, :1]), ahead[:, :-1]], axis=1)
    return behind - previous

def precondition(field, weights, ratio_real, ratio_imag):
    weighted = field * weights[None, :, None, None]
    spectrum = jnp.fft.fftn(weighted[0] + 1j * weighted[1], axes=(0, 1, 2))
    solved = spectrum * (ratio_real - 1j * ratio_imag)
    back = jnp.fft.ifftn(solved, axes=(0, 1, 2))
    result = jnp.stack([jnp.real(back), jnp.imag(back)]).astype(jnp.float32)
    return result / weights[None, :, None, None]

def least_squares(hessenberg, start):
    matrix = [list(line) for line in hessenberg]
    target = [start] + [jnp.zeros((), jnp.float32) for unused in range(ITERS)]
    cosines = []
    sines = []
    for column in range(ITERS):
        for row in range(column):
            upper = matrix[row][column]
            lower = matrix[row + 1][column]
            matrix[row][column] = cosines[row] * upper + sines[row] * lower
            matrix[row + 1][column] = -sines[row] * upper + cosines[row] * lower
        upper = matrix[column][column]
        lower = matrix[column + 1][column]
        radius = jnp.sqrt(upper * upper + lower * lower)
        cosines.append(upper / radius)
        sines.append(lower / radius)
        matrix[column][column] = radius
        target[column + 1] = -sines[column] * target[column]
        target[column] = cosines[column] * target[column]
    factors = [None] * ITERS
    for row in reversed(range(ITERS)):
        total = target[row]
        for other in range(row + 1, ITERS):
            total = total - matrix[row][other] * factors[other]
        factors[row] = total / matrix[row][row]
    return factors

def reference(u_init, phase, absorb):
    beta = jnp.float32(alpha) ** (1.0 / TIME)
    steps = jnp.arange(TIME).astype(jnp.float32)
    weights = jnp.float32(alpha) ** (steps / TIME)
    theta = steps * (2.0 * math.pi / TIME)
    cosine = (beta * jnp.cos(theta))[:, None, None]
    sine = (beta * jnp.sin(theta))[:, None, None]
    symbol_x = 4.0 * jnp.sin(jnp.arange(NX).astype(jnp.float32) * (math.pi / NX)) ** 2
    symbol_y = 4.0 * jnp.sin(jnp.arange(NY).astype(jnp.float32) * (math.pi / NY)) ** 2
    symbol = (symbol_x[:, None] + symbol_y[None, :])[None]
    eigen_real = 1.0 - cosine + tau * symbol * sine / 2.0
    eigen_imag = sine + tau * symbol * (1.0 + cosine) / 2.0
    modulus = eigen_real * eigen_real + eigen_imag * eigen_imag
    ratio_real = eigen_real / modulus
    ratio_imag = eigen_imag / modulus
    first = u_init + 0.5 * generator(u_init, phase, absorb)
    right_side = jnp.concatenate([first[:, None], jnp.zeros((2, TIME - 1, NX, NY), jnp.float32)], axis=1)
    start = jnp.sqrt(jnp.sum(right_side * right_side))
    basis = [right_side / start]
    corrected = []
    hessenberg = [[jnp.zeros((), jnp.float32) for unused in range(ITERS)] for other in range(ITERS + 1)]
    for column in range(ITERS):
        update = precondition(basis[column], weights, ratio_real, ratio_imag)
        corrected.append(update)
        image = operate(update, phase, absorb)
        products = [jnp.sum(image * vector) for vector in basis]
        for vector, amount in zip(basis, products):
            image = image - amount * vector
        length = jnp.sqrt(jnp.sum(image * image))
        for row in range(column + 1):
            hessenberg[row][column] = products[row]
        hessenberg[column + 1][column] = length
        if column + 1 < ITERS:
            basis.append(image / length)
    factors = least_squares(hessenberg, start)
    solution = jnp.zeros((2, TIME, NX, NY), jnp.float32)
    for amount, update in zip(factors, corrected):
        solution = solution + amount * update
    return solution
```

```python
import math

import jax
import jax.numpy as jnp
import numpy as np
from jax import lax
from jax.experimental import pallas as pl
from jax.experimental.pallas import tpu as pltpu
from jax.sharding import Mesh
from jax.sharding import PartitionSpec as P

NX = 512
NY = 512
HALF = 256
TIME = 64
ITERS = 4
DEVICES = 128
TM = ("tm_0", "tm_1", "tm_2", "tm_3")
TM_SPACE = ("tm_0", "tm_1", "tm_2", "tm_3", "space")

tau = 400.0
alpha = 0.4
shift = alpha * alpha / (1.0 - alpha * alpha)
scale = alpha / (1.0 - alpha * alpha)
highest = lax.Precision.HIGHEST
f32 = jnp.float32
bf16 = jnp.bfloat16


def dft_tables():
    mode = np.arange(HALF)[:, None]
    cell = np.arange(HALF)[None, :]
    stack = []
    for frequency, transposed in ((2 * mode, False), (2 * mode + 1, False), (2 * mode + 1, True)):
        angle = 2.0 * np.pi * ((frequency * cell) % NX) / NX
        parts = [np.cos(angle), np.sin(angle)]
        stack.append(np.concatenate([part.T if transposed else part for part in parts]))
    exact = np.stack(stack)
    high = exact.astype(bf16)
    low = (exact - high.astype(np.float64)).astype(bf16)
    return np.stack([high, low])


TABLES = dft_tables()
EVEN, ODD, ODD_T = 0, 1, 2


def halves(value):
    high = value.astype(bf16)
    return high, (value - high.astype(f32)).astype(bf16)


def dot(left, right):
    return jnp.dot(left, right, preferred_element_type=f32)


def table_times(table, which, value):
    high, low = halves(value)
    return dot(table[0, which], high) + dot(table[1, which], high) + dot(table[0, which], low)


def times_table(value, table, which):
    high, low = halves(value)
    return dot(high, table[0, which]) + dot(high, table[1, which]) + dot(low, table[0, which])


def upper_rows(shape):
    return lax.broadcasted_iota(jnp.int32, shape, len(shape) - 2) < 4


def swapped(value):
    return pltpu.roll(value, 4, value.ndim - 2)


def signs(shape, upper, lower):
    return jnp.where(upper_rows(shape), f32(upper), f32(lower))


def split_parts(block):
    pair = block.reshape(32, 2, 8, HALF)
    first, second = pair[:, 0], pair[:, 1]
    upper = upper_rows((1, 8, 1))
    real = jnp.where(upper, first, swapped(second))
    imag = jnp.where(upper, swapped(first), second)
    return real.reshape(HALF, HALF), imag.reshape(HALF, HALF)


def merge_parts(real, imag):
    real = real.reshape(32, 8, HALF)
    imag = imag.reshape(32, 8, HALF)
    upper = upper_rows((1, 8, 1))
    first = jnp.where(upper, real, swapped(imag))
    second = jnp.where(upper, swapped(real), imag)
    return jnp.stack([first, second], axis=1).reshape(64, 8, HALF)


def cells_kernel(arrived, damping, table, field, sent):
    def inverse(part, which):
        real, imag = split_parts(arrived[pl.ds(part * 64, 64)])
        product = table_times(table, which, jnp.concatenate([real, imag], axis=1))
        top, bottom = product[:HALF], product[HALF:]
        return top[:, :HALF] - bottom[:, HALF:], top[:, HALF:] + bottom[:, :HALF]

    even_real, even_imag = inverse(0, EVEN)
    odd_real, odd_imag = inverse(1, ODD_T)
    near = (even_real + odd_real, even_imag + odd_imag)
    far = (even_real - odd_real, even_imag - odd_imag)
    damped = []
    for place, (real, imag) in enumerate((near, far)):
        rows = pl.ds(place * HALF, HALF)
        field[0, rows] = real
        field[1, rows] = imag
        absorb = damping[0, rows]
        phase = damping[1, rows]
        damped.append((absorb * real - phase * imag, absorb * imag + phase * real))

    def forward(part, which, sign):
        value = jnp.concatenate(
            [damped[0][0] + sign * damped[1][0], damped[0][1] + sign * damped[1][1]], axis=1
        )
        product = table_times(table, which, value)
        top, bottom = product[:HALF], product[HALF:]
        sent[pl.ds(part * 64, 64)] = merge_parts(
            top[:, :HALF] + bottom[:, HALF:], top[:, HALF:] - bottom[:, :HALF]
        )

    forward(0, EVEN, 1.0)
    forward(1, ODD, -1.0)


def on_cells(arrived, damping, table):
    return pl.pallas_call(
        cells_kernel,
        out_shape=(
            jax.ShapeDtypeStruct((2, NY, HALF), f32),
            jax.ShapeDtypeStruct((DEVICES, 8, HALF), f32),
        ),
        name="cells",
    )(arrived, damping, table)


def product_of(real, signed_imag, value):
    return real * value + signed_imag * swapped(value)


def rotation(angle_tangent):
    side = signs((8, NX), -1.0, 1.0)
    inverse = 1.0 / (1.0 + angle_tangent * angle_tangent)
    return (
        (1.0 - angle_tangent * angle_tangent) * inverse,
        -2.0 * angle_tangent * inverse * side,
        inverse,
        -angle_tangent * inverse * side,
    )


def multiplied(left, right):
    return left[0] * right[0] - left[1] * right[1], left[0] * right[1] + left[1] * right[0]


def wrap_factor(turn):
    side = signs((8, NX), -1.0, 1.0)
    power = turn
    for unused in range(6):
        power = multiplied(power, power)
        power = (power[0], power[1])
    return power, side


def rows_forward(block, count, table, into):
    pair = block.reshape(count, 2, 8, HALF)
    first, second = pair[:, 0], pair[:, 1]
    side = signs((1, 8, 1), 1.0, -1.0)
    for value, which, start in ((first + second, EVEN, 0), (first - second, ODD_T, HALF)):
        value = jnp.concatenate([value, side * swapped(value)], axis=2).reshape(8 * count, NX)
        into[:, :, pl.ds(start, HALF)] = times_table(value, table, which).reshape(count, 8, HALF)


def rows_inverse(modes, table, sent):
    side = signs((1, 8, 1), -1.0, 1.0)
    results = []
    for which, start in ((EVEN, 0), (ODD, HALF)):
        value = modes[:, :, pl.ds(start, HALF)]
        value = jnp.concatenate([value, side * swapped(value)], axis=2).reshape(TIME * 8, NX)
        results.append(times_table(value, table, which).reshape(TIME, 8, HALF))
    even, odd = results
    sent[...] = jnp.stack([even + odd, even - odd], axis=1).reshape(DEVICES, 8, HALF)


def signed_power(turn, count):
    side = signs((8, NX), -1.0, 1.0)
    real, imag = turn[0], turn[1] * side
    for unused in range(count):
        real, imag = real * real - imag * imag, 2.0 * real * imag
    return real, imag, side


def closing(turn):
    real, imag, side = signed_power(turn, 6)
    real, imag = alpha * real, alpha * imag
    rest = 1.0 - real
    inverse = 1.0 / (rest * rest + imag * imag)
    return (real * rest - imag * imag) * inverse, (imag * rest + real * imag) * inverse * side


def next_power(power, turn, conjugate):
    sign = -1.0 if conjugate else 1.0
    real = power[0] * turn[0] - sign * power[1] * turn[1]
    imag = sign * power[0] * turn[1] + power[1] * turn[0]
    return real, imag


NORMAL = 1.0 / (NX * NY)


def replay(turn, offset, summed, modes):
    def step(n, power):
        value = offset if summed is None else offset + summed[n]
        modes[n] = NORMAL * product_of(power[0], power[1], value)
        return next_power(power, turn, False)

    one = jnp.ones((8, NX), f32)
    lax.fori_loop(0, TIME, step, (one, jnp.zeros((8, NX), f32)), unroll=4)


def opening_kernel(block, tangent, table, vector, offset, sent, spectrum, modes):
    rows_forward(block[...], 2, table, spectrum)
    slope = tangent[...]
    turn_real, turn_imag, gain_real, gain_imag = rotation(slope)
    side = signs((8, NX), -1.0, 1.0)
    wave, damped = spectrum[0], spectrum[1]
    vector[...] = product_of(1.0, -slope * side, wave) - damped
    value = product_of(turn_real, turn_imag, wave) - product_of(gain_real, gain_imag, damped)
    wrap = product_of(*closing((turn_real, turn_imag)), value)
    offset[...] = wrap
    replay((turn_real, turn_imag), wrap + value, None, modes)
    rows_inverse(modes, table, sent)


def opening(block, tangent, table):
    return pl.pallas_call(
        opening_kernel,
        out_shape=(
            jax.ShapeDtypeStruct((8, NX), f32),
            jax.ShapeDtypeStruct((8, NX), f32),
            jax.ShapeDtypeStruct((DEVICES, 8, HALF), f32),
        ),
        scratch_shapes=[pltpu.VMEM((2, 8, NX), f32), pltpu.VMEM((TIME, 8, NX), f32)],
        name="opening",
    )(block, tangent, table)


def image_step(n, before, spectrum, slope_signed, offset, earlier):
    here = spectrum[n]
    value = here + before
    if earlier is not None:
        value = value - shift * earlier[n]
    return here, value * (1.0 / scale)


def wrapped_term(slope, offset):
    side = signs((8, NX), -1.0, 1.0)
    return offset + slope * side * swapped(offset)


def modes_kernel_of(first):
    def body(block, tangent, table, earlier, offset_in, vector, offset, sent, spectrum, summed):
        rows_forward(block[...], TIME, table, spectrum)
        slope = tangent[...]
        turn_real, turn_imag, gain_real, gain_imag = rotation(slope)
        turn = (turn_real, turn_imag)
        wrap = wrapped_term(slope, offset_in[...])
        if first:
            wrap = wrap - shift * earlier[...]

        def step(n, carry):
            before, total, power = carry
            here, value = image_step(n, before, spectrum, None, None, None if first else earlier)
            vector[n] = value
            total = total + product_of(power[0], power[1], value)
            summed[n] = total
            return here, total, next_power(power, turn, True)

        zero = jnp.zeros((8, NX), f32)
        unused, total, power = lax.fori_loop(
            0, TIME, step, (wrap, zero, (gain_real, gain_imag)), unroll=4
        )
        wrap = product_of(*closing(turn), total)
        offset[...] = wrap
        replay(turn, wrap, summed, spectrum)
        rows_inverse(spectrum, table, sent)

    return body


def on_modes(block, tangent, table, earlier, offset_in, first):
    return pl.pallas_call(
        modes_kernel_of(first),
        out_shape=(
            jax.ShapeDtypeStruct((TIME, 8, NX), f32),
            jax.ShapeDtypeStruct((8, NX), f32),
            jax.ShapeDtypeStruct((DEVICES, 8, HALF), f32),
        ),
        scratch_shapes=[pltpu.VMEM((TIME, 8, NX), f32), pltpu.VMEM((TIME, 8, NX), f32)],
        name="modes",
    )(block, tangent, table, earlier, offset_in)


PAIRS = [(i, j) for i in range(1, ITERS + 1) for j in range(i, ITERS + 1)]


def products_kernel(block, tangent, table, w0, w1, w2, w3, offset_in, totals, spectrum):
    rows_forward(block[...], TIME, table, spectrum)
    wrap = wrapped_term(tangent[...], offset_in[...])

    def narrowed(value):
        return value[:, 0:128] + value[:, 128:256] + value[:, 256:384] + value[:, 384:512]

    def step(n, carry):
        before, sums = carry
        here, value = image_step(n, before, spectrum, None, None, w3)
        vectors = (None, w1[n], w2[n], w3[n], value)
        sums = tuple(
            total + narrowed(vectors[i] * vectors[j]) for total, (i, j) in zip(sums, PAIRS)
        )
        return here, sums

    zero = jnp.zeros((8, 128), f32)
    start = w0[...]
    here, first = image_step(0, wrap, spectrum, None, None, w3)
    heads = (start, w1[0], w2[0], w3[0], first)
    for i, vector in enumerate(heads):
        totals[i] = narrowed(start * vector)
    sums = tuple(narrowed(heads[i] * heads[j]) for i, j in PAIRS)
    unused, sums = lax.fori_loop(1, TIME, step, (here, sums), unroll=3)
    for place, total in enumerate(sums):
        totals[place + 5] = total
    totals[15] = zero


def products(block, tangent, table, vectors, offset_in):
    return pl.pallas_call(
        products_kernel,
        out_shape=jax.ShapeDtypeStruct((16, 8, 128), f32),
        scratch_shapes=[pltpu.VMEM((TIME, 8, NX), f32)],
        name="products",
    )(block, tangent, table, *vectors, offset_in)


def least_squares(gram):
    size = ITERS + 1
    root = [[None] * size for unused in range(size)]
    for i in range(size):
        for j in range(i, size):
            total = gram[i][j]
            for k in range(i):
                total = total - root[k][i] * root[k][j]
            root[i][j] = jnp.sqrt(total) if i == j else total / root[i][i]
    matrix = [[jnp.zeros_like(gram[0][0]) for unused in range(ITERS)] for other in range(size)]
    for column in range(ITERS):
        for row in range(column + 2):
            total = scale * root[row][column + 1]
            if row <= column:
                total = total + (1.0 + shift) * root[row][column]
            matrix[row][column] = total
    target = [root[0][0]] + [jnp.zeros_like(gram[0][0]) for unused in range(ITERS)]
    cosines = []
    sines = []
    for column in range(ITERS):
        for row in range(column):
            upper = matrix[row][column]
            lower = matrix[row + 1][column]
            matrix[row][column] = cosines[row] * upper + sines[row] * lower
            matrix[row + 1][column] = -sines[row] * upper + cosines[row] * lower
        upper = matrix[column][column]
        lower = matrix[column + 1][column]
        radius = jnp.sqrt(upper * upper + lower * lower)
        cosines.append(upper / radius)
        sines.append(lower / radius)
        matrix[column][column] = radius
        target[column + 1] = -sines[column] * target[column]
        target[column] = cosines[column] * target[column]
    factors = [None] * ITERS
    for row in reversed(range(ITERS)):
        total = target[row]
        for other in range(row + 1, ITERS):
            total = total - matrix[row][other] * factors[other]
        factors[row] = total / matrix[row][row]
    return factors


def combine_kernel(totals, z0, z1, z2, z3, out):
    summed = jnp.sum(totals[...], axis=0)
    size = ITERS + 1
    gram = [[None] * size for unused in range(size)]
    order = [(0, j) for j in range(size)] + PAIRS
    for place, (i, j) in enumerate(order):
        value = jnp.sum(summed[place : place + 1, :], axis=1, keepdims=True)
        gram[i][j] = value
        gram[j][i] = value
    factors = least_squares(gram)
    for part in range(2):
        value = factors[0] * z0[part]
        for factor, other in zip(factors[1:], (z1, z2, z3)):
            value = value + factor * other[part]
        out[part, 0] = value.T


def combine(totals, fields):
    return pl.pallas_call(
        combine_kernel,
        out_shape=jax.ShapeDtypeStruct((2, 1, HALF, NY), f32),
        name="combine",
    )(totals, *fields)


def exchange(value):
    return lax.all_to_all(value, TM_SPACE, split_axis=0, concat_axis=0, tiled=True)


def column_modes(first, count):
    order = first + jnp.arange(count, dtype=jnp.int32)
    return 2 * (order % HALF) + order // HALF


def shards(u_init, phase, absorb):
    step = lax.axis_index(TM)
    half = lax.axis_index("space")
    table = jnp.asarray(TABLES)
    damping = 0.5 * jnp.stack([absorb, phase])
    modes = column_modes(8 * step, 8)
    turns = modes[:, None] * jnp.arange(NY, dtype=jnp.int32)[None, :] % NY
    angle = turns.astype(f32) * (2.0 * math.pi / NY)
    damped = jnp.stack(
        [
            damping[0] * u_init[0] - damping[1] * u_init[1],
            damping[0] * u_init[1] + damping[1] * u_init[0],
        ]
    )
    fields = jnp.stack([u_init, damped])
    cosine = jnp.einsum("fcxy,ky->fckx", fields, jnp.cos(angle), precision=highest)
    sine = jnp.einsum("fcxy,ky->fckx", fields, jnp.sin(angle), precision=highest)
    columns = jnp.stack([cosine[:, 0] + sine[:, 1], cosine[:, 1] - sine[:, 0]], axis=1)
    columns = columns.reshape(2, 2, 2, 4, HALF)
    mine = lax.dynamic_index_in_dim(columns, half, 2, keepdims=False).reshape(2, 8, HALF)
    theirs = lax.dynamic_index_in_dim(columns, 1 - half, 2, keepdims=False).reshape(2, 8, HALF)
    theirs = lax.ppermute(theirs, "space", [(0, 1), (1, 0)])
    block = jnp.where(
        half == 0, jnp.stack([mine, theirs], axis=1), jnp.stack([theirs, mine], axis=1)
    ).reshape(4, 8, HALF)
    own = column_modes(8 * step + 4 * half, 4).astype(f32)
    rows = jnp.arange(HALF, dtype=jnp.int32)
    rows = jnp.concatenate([2 * rows, 2 * rows + 1]).astype(f32)
    symbol_y = 4.0 * jnp.sin(own * (math.pi / NY)) ** 2
    symbol_x = 4.0 * jnp.sin(rows * (math.pi / NX)) ** 2
    tangent = (0.5 * tau) * (jnp.concatenate([symbol_y, symbol_y])[:, None] + symbol_x[None, :])
    damping = damping.swapaxes(1, 2)

    vector, offset, sent = opening(block, tangent, table)
    vectors = [vector]
    found = []
    for column in range(ITERS):
        field, sent = on_cells(exchange(sent), damping, table)
        found.append(field)
        arrived = exchange(sent)
        if column + 1 < ITERS:
            vector, offset, sent = on_modes(
                arrived, tangent, table, vectors[-1], offset, column == 0
            )
            vectors.append(vector)
    totals = products(arrived, tangent, table, vectors, offset)
    totals = jnp.sum(totals, axis=1)
    spread = jnp.broadcast_to(totals[None], (DEVICES, 16, 128))
    return combine(exchange(spread), found)


def solution(mesh):
    torus = Mesh(
        mesh.devices.reshape(4, 4, 2, 2, mesh.shape["space"]),
        ("tm_0", "tm_1", "tm_2", "tm_3", "space"),
    )
    placed = (P(None, "space", None), P("space", None), P("space", None))
    return jax.shard_map(
        shards, mesh=torus, in_specs=placed, out_specs=P(None, TM, "space", None), check_vma=False
    )
```

```python
import math

import jax
import jax.numpy as jnp
import numpy as np
from jax import lax
from jax.experimental import pallas as pl
from jax.experimental.pallas import tpu as pltpu
from jax.sharding import Mesh
from jax.sharding import PartitionSpec as P

NX = 512
NY = 512
HALF = 256
TIME = 64
ITERS = 4
DEVICES = 128
TM = ("tm_0", "tm_1", "tm_2", "tm_3")
TM_SPACE = ("tm_0", "tm_1", "tm_2", "tm_3", "space")

tau = 400.0
alpha = 0.4
shift = alpha * alpha / (1.0 - alpha * alpha)
scale = alpha / (1.0 - alpha * alpha)
highest = lax.Precision.HIGHEST
f32 = jnp.float32
bf16 = jnp.bfloat16


def dft_tables():
    mode = np.arange(HALF)[:, None]
    cell = np.arange(HALF)[None, :]
    stack = []
    for frequency, transposed in ((2 * mode, False), (2 * mode + 1, False), (2 * mode + 1, True)):
        angle = 2.0 * np.pi * ((frequency * cell) % NX) / NX
        parts = [np.cos(angle), np.sin(angle)]
        stack.append(np.concatenate([part.T if transposed else part for part in parts]))
    exact = np.stack(stack)
    high = exact.astype(bf16)
    low = (exact - high.astype(np.float64)).astype(bf16)
    return np.stack([high, low])


TABLES = dft_tables()
EVEN, ODD, ODD_T = 0, 1, 2


def halves(value):
    high = value.astype(bf16)
    return high, (value - high.astype(f32)).astype(bf16)


def dot(left, right):
    return jnp.dot(left, right, preferred_element_type=f32)


def table_times(table, which, value):
    high, low = halves(value)
    return dot(table[0, which], high) + dot(table[1, which], high) + dot(table[0, which], low)


def times_table(value, table, which):
    high, low = halves(value)
    return dot(high, table[0, which]) + dot(high, table[1, which]) + dot(low, table[0, which])


def call(body, out_shape, name, scratch, *operands):
    inside = pl.BlockSpec(memory_space=pltpu.VMEM)
    return pl.pallas_call(
        body,
        out_shape=out_shape,
        in_specs=[inside] * len(operands),
        out_specs=jax.tree.map(lambda unused: inside, out_shape),
        scratch_shapes=scratch,
        compiler_params=pltpu.CompilerParams(vmem_limit_bytes=24 << 20),
        name=name,
    )(*operands)


def array(*shape):
    return jax.ShapeDtypeStruct(shape, f32)


def upper_rows(shape):
    return lax.broadcasted_iota(jnp.int32, shape, len(shape) - 2) < 4


def swapped(value):
    return pltpu.roll(value, 4, value.ndim - 2)


def signs(shape, upper, lower):
    return jnp.where(upper_rows(shape), f32(upper), f32(lower))


def split_parts(block):
    pair = block.reshape(32, 2, 8, HALF)
    first, second = pair[:, 0], pair[:, 1]
    upper = upper_rows((1, 8, 1))
    real = jnp.where(upper, first, swapped(second))
    imag = jnp.where(upper, swapped(first), second)
    return real.reshape(HALF, HALF), imag.reshape(HALF, HALF)


def merge_parts(real, imag):
    real = real.reshape(32, 8, HALF)
    imag = imag.reshape(32, 8, HALF)
    upper = upper_rows((1, 8, 1))
    first = jnp.where(upper, real, swapped(imag))
    second = jnp.where(upper, swapped(real), imag)
    return jnp.stack([first, second], axis=1).reshape(64, 8, HALF)


def cells_kernel(arrived, damping, table, field, sent):
    def inverse(part, which):
        real, imag = split_parts(arrived[pl.ds(part * 64, 64)])
        product = table_times(table, which, jnp.concatenate([real, imag], axis=1))
        top, bottom = product[:HALF], product[HALF:]
        return top[:, :HALF] - bottom[:, HALF:], top[:, HALF:] + bottom[:, :HALF]

    even_real, even_imag = inverse(0, EVEN)
    odd_real, odd_imag = inverse(1, ODD_T)
    near = (even_real + odd_real, even_imag + odd_imag)
    far = (even_real - odd_real, even_imag - odd_imag)
    damped = []
    for place, (real, imag) in enumerate((near, far)):
        rows = pl.ds(place * HALF, HALF)
        field[0, rows] = real
        field[1, rows] = imag
        absorb = damping[0, rows]
        phase = damping[1, rows]
        damped.append((absorb * real - phase * imag, absorb * imag + phase * real))

    def forward(part, which, sign):
        value = jnp.concatenate(
            [damped[0][0] + sign * damped[1][0], damped[0][1] + sign * damped[1][1]], axis=1
        )
        product = table_times(table, which, value)
        top, bottom = product[:HALF], product[HALF:]
        sent[pl.ds(part * 64, 64)] = merge_parts(
            top[:, :HALF] + bottom[:, HALF:], top[:, HALF:] - bottom[:, :HALF]
        )

    forward(0, EVEN, 1.0)
    forward(1, ODD, -1.0)


def on_cells(arrived, damping, table):
    shapes = (array(2, NY, HALF), array(DEVICES, 8, HALF))
    return call(cells_kernel, shapes, "cells", (), arrived, damping, table)


def product_of(real, signed_imag, value):
    return real * value + signed_imag * swapped(value)


def rotation(angle_tangent):
    side = signs((8, NX), -1.0, 1.0)
    inverse = 1.0 / (1.0 + angle_tangent * angle_tangent)
    return (
        (1.0 - angle_tangent * angle_tangent) * inverse,
        -2.0 * angle_tangent * inverse * side,
        inverse,
        -angle_tangent * inverse * side,
    )


def multiplied(left, right):
    return left[0] * right[0] - left[1] * right[1], left[0] * right[1] + left[1] * right[0]


def wrap_factor(turn):
    side = signs((8, NX), -1.0, 1.0)
    power = turn
    for unused in range(6):
        power = multiplied(power, power)
        power = (power[0], power[1])
    return power, side


def rows_forward(block, count, table, into):
    pair = block.reshape(count, 2, 8, HALF)
    first, second = pair[:, 0], pair[:, 1]
    side = signs((1, 8, 1), 1.0, -1.0)
    for value, which, start in ((first + second, EVEN, 0), (first - second, ODD_T, HALF)):
        value = jnp.concatenate([value, side * swapped(value)], axis=2).reshape(8 * count, NX)
        into[:, :, pl.ds(start, HALF)] = times_table(value, table, which).reshape(count, 8, HALF)


def rows_inverse(modes, table, sent):
    side = signs((1, 8, 1), -1.0, 1.0)
    results = []
    for which, start in ((EVEN, 0), (ODD, HALF)):
        value = modes[:, :, pl.ds(start, HALF)]
        value = jnp.concatenate([value, side * swapped(value)], axis=2).reshape(TIME * 8, NX)
        results.append(times_table(value, table, which).reshape(TIME, 8, HALF))
    even, odd = results
    sent[...] = jnp.stack([even + odd, even - odd], axis=1).reshape(DEVICES, 8, HALF)


def signed_power(turn, count):
    side = signs((8, NX), -1.0, 1.0)
    real, imag = turn[0], turn[1] * side
    for unused in range(count):
        real, imag = real * real - imag * imag, 2.0 * real * imag
    return real, imag, side


def closing(turn):
    real, imag, side = signed_power(turn, 6)
    real, imag = alpha * real, alpha * imag
    rest = 1.0 - real
    inverse = 1.0 / (rest * rest + imag * imag)
    return (real * rest - imag * imag) * inverse, (imag * rest + real * imag) * inverse * side


def next_power(power, turn, conjugate):
    sign = -1.0 if conjugate else 1.0
    real = power[0] * turn[0] - sign * power[1] * turn[1]
    imag = sign * power[0] * turn[1] + power[1] * turn[0]
    return real, imag


NORMAL = 1.0 / (NX * NY)


def replay(turn, offset, summed, modes):
    def step(n, power):
        value = offset if summed is None else offset + summed[n]
        modes[n] = NORMAL * product_of(power[0], power[1], value)
        return next_power(power, turn, False)

    one = jnp.ones((8, NX), f32)
    lax.fori_loop(0, TIME, step, (one, jnp.zeros((8, NX), f32)), unroll=4)


def opening_kernel(block, tangent, table, vector, offset, sent, spectrum, modes):
    rows_forward(block[...], 2, table, spectrum)
    slope = tangent[...]
    turn_real, turn_imag, gain_real, gain_imag = rotation(slope)
    side = signs((8, NX), -1.0, 1.0)
    wave, damped = spectrum[0], spectrum[1]
    vector[...] = product_of(1.0, -slope * side, wave) - damped
    value = product_of(turn_real, turn_imag, wave) - product_of(gain_real, gain_imag, damped)
    wrap = product_of(*closing((turn_real, turn_imag)), value)
    offset[...] = wrap
    replay((turn_real, turn_imag), wrap + value, None, modes)
    rows_inverse(modes, table, sent)


def opening(block, tangent, table):
    shapes = (array(8, NX), array(8, NX), array(DEVICES, 8, HALF))
    scratch = (pltpu.VMEM((2, 8, NX), f32), pltpu.VMEM((TIME, 8, NX), f32))
    return call(opening_kernel, shapes, "opening", scratch, block, tangent, table)


def image_step(n, before, spectrum, slope_signed, offset, earlier):
    here = spectrum[n]
    value = here + before
    if earlier is not None:
        value = value - shift * earlier[n]
    return here, value * (1.0 / scale)


def wrapped_term(slope, offset):
    side = signs((8, NX), -1.0, 1.0)
    return offset + slope * side * swapped(offset)


def modes_kernel_of(first):
    def body(block, tangent, table, earlier, offset_in, vector, offset, sent, spectrum, summed):
        rows_forward(block[...], TIME, table, spectrum)
        slope = tangent[...]
        turn_real, turn_imag, gain_real, gain_imag = rotation(slope)
        turn = (turn_real, turn_imag)
        wrap = wrapped_term(slope, offset_in[...])
        if first:
            wrap = wrap - shift * earlier[...]

        def step(n, carry):
            before, total, power = carry
            here, value = image_step(n, before, spectrum, None, None, None if first else earlier)
            vector[n] = value
            total = total + product_of(power[0], power[1], value)
            summed[n] = total
            return here, total, next_power(power, turn, True)

        zero = jnp.zeros((8, NX), f32)
        unused, total, power = lax.fori_loop(
            0, TIME, step, (wrap, zero, (gain_real, gain_imag)), unroll=4
        )
        wrap = product_of(*closing(turn), total)
        offset[...] = wrap
        replay(turn, wrap, summed, spectrum)
        rows_inverse(spectrum, table, sent)

    return body


def on_modes(block, tangent, table, earlier, offset_in, first):
    shapes = (array(TIME, 8, NX), array(8, NX), array(DEVICES, 8, HALF))
    scratch = (pltpu.VMEM((TIME, 8, NX), f32), pltpu.VMEM((TIME, 8, NX), f32))
    body = modes_kernel_of(first)
    return call(body, shapes, "modes", scratch, block, tangent, table, earlier, offset_in)


PAIRS = [(i, j) for i in range(1, ITERS + 1) for j in range(i, ITERS + 1)]


def products_kernel(block, tangent, table, w0, w1, w2, w3, offset_in, totals, spectrum):
    rows_forward(block[...], TIME, table, spectrum)
    wrap = wrapped_term(tangent[...], offset_in[...])

    def narrowed(value):
        return value[:, 0:128] + value[:, 128:256] + value[:, 256:384] + value[:, 384:512]

    def step(n, carry):
        before, sums = carry
        here, value = image_step(n, before, spectrum, None, None, w3)
        vectors = (None, w1[n], w2[n], w3[n], value)
        sums = tuple(
            total + narrowed(vectors[i] * vectors[j]) for total, (i, j) in zip(sums, PAIRS)
        )
        return here, sums

    start = w0[...]
    here, first = image_step(0, wrap, spectrum, None, None, w3)
    heads = (start, w1[0], w2[0], w3[0], first)
    sums = tuple(narrowed(heads[i] * heads[j]) for i, j in PAIRS)
    unused, sums = lax.fori_loop(1, TIME, step, (here, sums), unroll=3)
    sums = tuple(narrowed(start * vector) for vector in heads) + sums
    lane = lax.broadcasted_iota(jnp.int32, (1, 128), 1)
    packed = jnp.zeros((1, 128), f32)
    for place, total in enumerate(sums):
        total = jnp.sum(jnp.sum(total, axis=0, keepdims=True), axis=1, keepdims=True)
        packed = jnp.where(lane == place, total, packed)
    totals[...] = packed


def products(block, tangent, table, vectors, offset_in):
    scratch = (pltpu.VMEM((TIME, 8, NX), f32),)
    operands = (block, tangent, table, *vectors, offset_in)
    return call(products_kernel, array(1, 128), "products", scratch, *operands)


def least_squares(gram):
    size = ITERS + 1
    root = [[None] * size for unused in range(size)]
    for i in range(size):
        for j in range(i, size):
            total = gram[i][j]
            for k in range(i):
                total = total - root[k][i] * root[k][j]
            root[i][j] = jnp.sqrt(total) if i == j else total / root[i][i]
    matrix = [[jnp.zeros_like(gram[0][0]) for unused in range(ITERS)] for other in range(size)]
    for column in range(ITERS):
        for row in range(column + 2):
            total = scale * root[row][column + 1]
            if row <= column:
                total = total + (1.0 + shift) * root[row][column]
            matrix[row][column] = total
    target = [root[0][0]] + [jnp.zeros_like(gram[0][0]) for unused in range(ITERS)]
    cosines = []
    sines = []
    for column in range(ITERS):
        for row in range(column):
            upper = matrix[row][column]
            lower = matrix[row + 1][column]
            matrix[row][column] = cosines[row] * upper + sines[row] * lower
            matrix[row + 1][column] = -sines[row] * upper + cosines[row] * lower
        upper = matrix[column][column]
        lower = matrix[column + 1][column]
        radius = jnp.sqrt(upper * upper + lower * lower)
        cosines.append(upper / radius)
        sines.append(lower / radius)
        matrix[column][column] = radius
        target[column + 1] = -sines[column] * target[column]
        target[column] = cosines[column] * target[column]
    factors = [None] * ITERS
    for row in reversed(range(ITERS)):
        total = target[row]
        for other in range(row + 1, ITERS):
            total = total - matrix[row][other] * factors[other]
        factors[row] = total / matrix[row][row]
    return factors


def combine_kernel(totals, z0, z1, z2, z3, out):
    summed = jnp.sum(totals[...], axis=0, keepdims=True)
    size = ITERS + 1
    gram = [[None] * size for unused in range(size)]
    lane = lax.broadcasted_iota(jnp.int32, (1, 128), 1)
    order = [(0, j) for j in range(size)] + PAIRS
    for place, (i, j) in enumerate(order):
        value = jnp.sum(jnp.where(lane == place, summed, 0.0), axis=1, keepdims=True)
        gram[i][j] = value
        gram[j][i] = value
    factors = least_squares(gram)
    for part in range(2):
        value = factors[0] * z0[part]
        for factor, other in zip(factors[1:], (z1, z2, z3)):
            value = value + factor * other[part]
        out[part, 0] = value.T


def combine(totals, fields):
    return call(combine_kernel, array(2, 1, HALF, NY), "combine", (), totals, *fields)


def exchange(value):
    return lax.all_to_all(value, TM_SPACE, split_axis=0, concat_axis=0, tiled=True)


def column_modes(first, count):
    order = first + jnp.arange(count, dtype=jnp.int32)
    return 2 * (order % HALF) + order // HALF


def shards(u_init, phase, absorb):
    step = lax.axis_index(TM)
    half = lax.axis_index("space")
    table = jnp.asarray(TABLES)
    damping = 0.5 * jnp.stack([absorb, phase])
    modes = column_modes(8 * step, 8)
    turns = modes[:, None] * jnp.arange(NY, dtype=jnp.int32)[None, :] % NY
    angle = turns.astype(f32) * (2.0 * math.pi / NY)
    damped = jnp.stack(
        [
            damping[0] * u_init[0] - damping[1] * u_init[1],
            damping[0] * u_init[1] + damping[1] * u_init[0],
        ]
    )
    fields = jnp.stack([u_init, damped])
    cosine = jnp.einsum("fcxy,ky->fckx", fields, jnp.cos(angle), precision=highest)
    sine = jnp.einsum("fcxy,ky->fckx", fields, jnp.sin(angle), precision=highest)
    columns = jnp.stack([cosine[:, 0] + sine[:, 1], cosine[:, 1] - sine[:, 0]], axis=1)
    columns = columns.reshape(2, 2, 2, 4, HALF)
    mine = lax.dynamic_index_in_dim(columns, half, 2, keepdims=False).reshape(2, 8, HALF)
    theirs = lax.dynamic_index_in_dim(columns, 1 - half, 2, keepdims=False).reshape(2, 8, HALF)
    theirs = lax.ppermute(theirs, "space", [(0, 1), (1, 0)])
    block = jnp.where(
        half == 0, jnp.stack([mine, theirs], axis=1), jnp.stack([theirs, mine], axis=1)
    ).reshape(4, 8, HALF)
    own = column_modes(8 * step + 4 * half, 4).astype(f32)
    rows = jnp.arange(HALF, dtype=jnp.int32)
    rows = jnp.concatenate([2 * rows, 2 * rows + 1]).astype(f32)
    symbol_y = 4.0 * jnp.sin(own * (math.pi / NY)) ** 2
    symbol_x = 4.0 * jnp.sin(rows * (math.pi / NX)) ** 2
    tangent = (0.5 * tau) * (jnp.concatenate([symbol_y, symbol_y])[:, None] + symbol_x[None, :])
    damping = damping.swapaxes(1, 2)

    vector, offset, sent = opening(block, tangent, table)
    vectors = [vector]
    found = []
    for column in range(ITERS):
        field, sent = on_cells(exchange(sent), damping, table)
        found.append(field)
        arrived = exchange(sent)
        if column + 1 < ITERS:
            vector, offset, sent = on_modes(
                arrived, tangent, table, vectors[-1], offset, column == 0
            )
            vectors.append(vector)
    totals = products(arrived, tangent, table, vectors, offset)
    return combine(exchange(jnp.broadcast_to(totals, (DEVICES, 128))), found)


def solution(mesh):
    torus = Mesh(
        mesh.devices.reshape(4, 4, 2, 2, mesh.shape["space"]),
        ("tm_0", "tm_1", "tm_2", "tm_3", "space"),
    )
    placed = (P(None, "space", None), P("space", None), P("space", None))
    return jax.shard_map(
        shards, mesh=torus, in_specs=placed, out_specs=P(None, TM, "space", None), check_vma=False
    )
```

```python
import math

import jax
import jax.numpy as jnp
import numpy as np
from jax import lax
from jax.experimental import pallas as pl
from jax.experimental.pallas import tpu as pltpu
from jax.sharding import Mesh
from jax.sharding import PartitionSpec as P

NX = 512
NY = 512
HALF = 256
TIME = 64
ITERS = 4
DEVICES = 128
TM = ("tm_0", "tm_1", "tm_2", "tm_3")
TM_SPACE = ("tm_0", "tm_1", "tm_2", "tm_3", "space")

tau = 400.0
alpha = 0.4
shift = alpha * alpha / (1.0 - alpha * alpha)
scale = alpha / (1.0 - alpha * alpha)
f32 = jnp.float32
bf16 = jnp.bfloat16


def dft_tables():
    mode = np.arange(HALF)[:, None]
    cell = np.arange(HALF)[None, :]
    stack = []
    for frequency, transposed in ((2 * mode, False), (2 * mode + 1, False), (2 * mode + 1, True)):
        angle = 2.0 * np.pi * ((frequency * cell) % NX) / NX
        parts = [np.cos(angle), np.sin(angle)]
        stack.append(np.concatenate([part.T if transposed else part for part in parts]))
    exact = np.stack(stack)
    high = exact.astype(bf16)
    low = (exact - high.astype(np.float64)).astype(bf16)
    return np.stack([high, low])


TABLES = dft_tables()
EVEN, ODD, ODD_T = 0, 1, 2


def halves(value):
    high = value.astype(bf16)
    return high, (value - high.astype(f32)).astype(bf16)


def dot(left, right):
    return jnp.dot(left, right, preferred_element_type=f32)


def dot_last(left, right):
    return lax.dot_general(left, right, (((1,), (1,)), ((), ())), preferred_element_type=f32)


def table_times(table, which, value):
    high, low = halves(value)
    return dot(table[0, which], high) + dot(table[1, which], high) + dot(table[0, which], low)


def times_table(value, table, which):
    high, low = halves(value)
    return dot(high, table[0, which]) + dot(high, table[1, which]) + dot(low, table[0, which])


def call(body, out_shape, name, scratch, *operands, copied=0):
    inside = pl.BlockSpec(memory_space=pltpu.VMEM)
    return pl.pallas_call(
        body,
        out_shape=out_shape,
        in_specs=[pl.BlockSpec(memory_space=pltpu.HBM)] * copied + [inside] * (len(operands) - copied),
        out_specs=jax.tree.map(lambda unused: inside, out_shape),
        scratch_shapes=scratch,
        compiler_params=pltpu.CompilerParams(vmem_limit_bytes=(63 if copied else 24) << 20),
        name=name,
    )(*operands)


def array(*shape):
    return jax.ShapeDtypeStruct(shape, f32)


def upper_rows(shape):
    return lax.broadcasted_iota(jnp.int32, shape, len(shape) - 2) < 4


def swapped(value):
    return pltpu.roll(value, 4, value.ndim - 2)


def signs(shape, upper, lower):
    return jnp.where(upper_rows(shape), f32(upper), f32(lower))


def split_parts(block):
    pair = block.reshape(32, 2, 8, HALF)
    first, second = pair[:, 0], pair[:, 1]
    upper = upper_rows((1, 8, 1))
    real = jnp.where(upper, first, swapped(second))
    imag = jnp.where(upper, swapped(first), second)
    return real.reshape(HALF, HALF), imag.reshape(HALF, HALF)


def merge_parts(real, imag):
    real = real.reshape(32, 8, HALF)
    imag = imag.reshape(32, 8, HALF)
    upper = upper_rows((1, 8, 1))
    first = jnp.where(upper, real, swapped(imag))
    second = jnp.where(upper, swapped(real), imag)
    return jnp.stack([first, second], axis=1).reshape(64, 8, HALF)


def cells_kernel(arrived, damping, table, field, sent):
    def inverse(part, which):
        real, imag = split_parts(arrived[pl.ds(part * 64, 64)])
        product = table_times(table, which, jnp.concatenate([real, imag], axis=1))
        top, bottom = product[:HALF], product[HALF:]
        return top[:, :HALF] - bottom[:, HALF:], top[:, HALF:] + bottom[:, :HALF]

    even_real, even_imag = inverse(0, EVEN)
    odd_real, odd_imag = inverse(1, ODD_T)
    near = (even_real + odd_real, even_imag + odd_imag)
    far = (even_real - odd_real, even_imag - odd_imag)
    damped = []
    for place, (real, imag) in enumerate((near, far)):
        rows = pl.ds(place * HALF, HALF)
        field[0, rows] = real
        field[1, rows] = imag
        absorb = damping[0, rows]
        phase = damping[1, rows]
        damped.append((absorb * real - phase * imag, absorb * imag + phase * real))

    def forward(part, which, sign):
        value = jnp.concatenate(
            [damped[0][0] + sign * damped[1][0], damped[0][1] + sign * damped[1][1]], axis=1
        )
        product = table_times(table, which, value)
        top, bottom = product[:HALF], product[HALF:]
        sent[pl.ds(part * 64, 64)] = merge_parts(
            top[:, :HALF] + bottom[:, HALF:], top[:, HALF:] - bottom[:, :HALF]
        )

    forward(0, EVEN, 1.0)
    forward(1, ODD, -1.0)


def on_cells(arrived, damping, table):
    shapes = (array(2, NY, HALF), array(DEVICES, 8, HALF))
    return call(cells_kernel, shapes, "cells", (), arrived, damping, table)


def product_of(real, signed_imag, value):
    return real * value + signed_imag * swapped(value)


def rotation(angle_tangent):
    side = signs((8, NX), -1.0, 1.0)
    inverse = 1.0 / (1.0 + angle_tangent * angle_tangent)
    return (
        (1.0 - angle_tangent * angle_tangent) * inverse,
        -2.0 * angle_tangent * inverse * side,
        inverse,
        -angle_tangent * inverse * side,
    )


def multiplied(left, right):
    return left[0] * right[0] - left[1] * right[1], left[0] * right[1] + left[1] * right[0]


def rows_forward(block, count, table, into):
    pair = block.reshape(count, 2, 8, HALF)
    first, second = pair[:, 0], pair[:, 1]
    side = signs((1, 8, 1), 1.0, -1.0)
    for value, which, start in ((first + second, EVEN, 0), (first - second, ODD_T, HALF)):
        value = jnp.concatenate([value, side * swapped(value)], axis=2).reshape(8 * count, NX)
        into[:, :, pl.ds(start, HALF)] = times_table(value, table, which).reshape(count, 8, HALF)


def rows_inverse(modes, table, sent):
    side = signs((1, 8, 1), -1.0, 1.0)
    results = []
    for which, start in ((EVEN, 0), (ODD, HALF)):
        value = modes[:, :, pl.ds(start, HALF)]
        value = jnp.concatenate([value, side * swapped(value)], axis=2).reshape(TIME * 8, NX)
        results.append(times_table(value, table, which).reshape(TIME, 8, HALF))
    even, odd = results
    sent[...] = jnp.stack([even + odd, even - odd], axis=1).reshape(DEVICES, 8, HALF)


def signed_power(turn, count):
    side = signs((8, NX), -1.0, 1.0)
    real, imag = turn[0], turn[1] * side
    for unused in range(count):
        real, imag = real * real - imag * imag, 2.0 * real * imag
    return real, imag, side


def closing(turn):
    real, imag, side = signed_power(turn, 6)
    real, imag = alpha * real, alpha * imag
    rest = 1.0 - real
    inverse = 1.0 / (rest * rest + imag * imag)
    return (real * rest - imag * imag) * inverse, (imag * rest + real * imag) * inverse * side


NORMAL = 1.0 / (NX * NY)


def fetched(sources, targets, arrivals):
    pieces = []
    for source, target in zip(sources, targets):
        for start in range(0, HALF, 64):
            if len(source.shape) == 3:
                pieces += [(source.at[c, pl.ds(start, 64)], target.at[c, pl.ds(start, 64)]) for c in range(2)]
            else:
                pieces.append((source.at[pl.ds(start, 64)], target.at[pl.ds(start, 64)]))
    copies = [
        pltpu.make_async_copy(source, target, arrivals.at[place])
        for place, (source, target) in enumerate(pieces)
    ]
    for copy in copies:
        copy.start()
    for copy in copies:
        copy.wait()


def columns_kernel(far_field, far_phase, far_absorb, trig, mine, theirs, field, phase, absorb, arrivals):
    fetched((far_field, far_phase, far_absorb), (field, phase, absorb), arrivals)
    real, imag = field[0], field[1]
    damped_real = 0.5 * (absorb[...] * real - phase[...] * imag)
    damped_imag = 0.5 * (absorb[...] * imag + phase[...] * real)
    high, low = halves(jnp.concatenate([real, imag, damped_real, damped_imag], axis=0))
    trig_high, trig_low = halves(trig[...])
    product = dot_last(trig_high, high) + dot_last(trig_low, high) + dot_last(trig_high, low)
    upper = upper_rows((8, 1))
    for place in range(2):
        start = 2 * place * HALF
        first = product[:, start : start + HALF]
        second = product[:, start + HALF : start + 2 * HALF]
        real = first[:8] + second[8:]
        imag = second[:8] - first[8:]
        mine[place] = jnp.where(upper, real, swapped(imag))
        theirs[place] = jnp.where(upper, swapped(real), imag)


def columns_of(field, phase, absorb, trig):
    operands = (field, phase, absorb, trig)
    scratch = (
        pltpu.VMEM((2, HALF, NY), f32),
        pltpu.VMEM((HALF, NY), f32),
        pltpu.VMEM((HALF, NY), f32),
        pltpu.SemaphoreType.DMA((16,)),
    )
    shapes = (array(2, 8, HALF), array(2, 8, HALF))
    return call(columns_kernel, shapes, "columns", scratch, *operands, copied=3)


def turning_kernel(phase, absorb, damping):
    damping[0] = (0.5 / scale) * absorb[...].T
    damping[1] = (0.5 / scale) * phase[...].T


def turned(phase, absorb):
    return call(turning_kernel, array(2, NY, HALF), "turning", (), phase, absorb)


def opening_kernel(block, tangent, table, vector, offset, sent, powers, spectrum, modes):
    rows_forward(block[...], 2, table, spectrum)
    slope = tangent[...]
    turn_real, turn_imag, gain_real, gain_imag = rotation(slope)
    side = signs((8, NX), -1.0, 1.0)
    wave, damped = spectrum[0], spectrum[1]
    vector[...] = product_of(1.0, -slope * side, wave) - damped
    value = product_of(turn_real, turn_imag, wave) - product_of(gain_real, gain_imag, damped)
    wrap = product_of(*closing((turn_real, turn_imag)), value)
    offset[...] = product_of(1.0, slope * side, wrap)
    start = NORMAL * (wrap + value)

    def step(n, power):
        real, imag = power
        powers[n, 0] = real
        powers[n, 1] = imag
        modes[n] = product_of(real, imag, start)
        return real * turn_real - imag * turn_imag, real * turn_imag + imag * turn_real

    one = jnp.ones((8, NX), f32)
    lax.fori_loop(0, TIME, step, (one, jnp.zeros((8, NX), f32)), unroll=4)
    rows_inverse(modes, table, sent)


def opening(block, tangent, table):
    shapes = (
        array(8, NX),
        array(8, NX),
        array(DEVICES, 8, HALF),
        array(TIME, 2, 8, NX),
    )
    scratch = (pltpu.VMEM((2, 8, NX), f32), pltpu.VMEM((TIME, 8, NX), f32))
    return call(opening_kernel, shapes, "opening", scratch, block, tangent, table)


def modes_kernel_of(first):
    def body(block, tangent, table, powers, earlier, wrap_in, vector, wrap_out, sent, modes, sums):
        rows_forward(block[...], TIME, table, modes)
        slope = tangent[...]
        turn_real, turn_imag, gain_real, gain_imag = rotation(slope)
        before = (1.0 / scale) * wrap_in[...]
        if first:
            before = before - alpha * earlier[...]

        def step(n, carry):
            before, total = carry
            here = modes[n]
            value = here + before
            if not first:
                value = value - alpha * earlier[n]
            vector[n] = value
            total = total + product_of(powers[n, 0], -powers[n, 1], value)
            sums[n] = total
            return here, total

        zero = jnp.zeros((8, NX), f32)
        unused, total = lax.fori_loop(0, TIME, step, (before, zero), unroll=4)
        wrap = product_of(*closing((turn_real, turn_imag)), total)
        wrap_out[...] = wrap
        gain_real, gain_imag = NORMAL * gain_real, NORMAL * gain_imag

        def replay(n, carry):
            value = product_of(gain_real, gain_imag, wrap + sums[n])
            modes[n] = product_of(powers[n, 0], powers[n, 1], value)
            return carry

        lax.fori_loop(0, TIME, replay, 0, unroll=4)
        rows_inverse(modes, table, sent)

    return body


def on_modes(block, tangent, table, powers, earlier, wrap, first):
    shapes = (array(TIME, 8, NX), array(8, NX), array(DEVICES, 8, HALF))
    scratch = (pltpu.VMEM((TIME, 8, NX), f32), pltpu.VMEM((TIME, 8, NX), f32))
    body = modes_kernel_of(first)
    operands = (block, tangent, table, powers, earlier, wrap)
    return call(body, shapes, "modes", scratch, *operands)


PAIRS = [(i, j) for i in range(1, ITERS + 1) for j in range(i, ITERS + 1)]


def products_kernel(block, table, w0, w1, w2, w3, wrap, totals, spectrum):
    rows_forward(block[...], TIME, table, spectrum)

    def narrowed(value):
        return value[:, 0:128] + value[:, 128:256] + value[:, 256:384] + value[:, 384:512]

    def step(n, carry):
        before, sums = carry
        here = spectrum[n]
        value = here + before - alpha * w3[n]
        vectors = (None, w1[n], w2[n], w3[n], value)
        sums = tuple(
            total + narrowed(vectors[i] * vectors[j]) for total, (i, j) in zip(sums, PAIRS)
        )
        return here, sums

    start = w0[...]
    here = spectrum[0]
    first = here + (1.0 / scale) * wrap[...] - alpha * w3[0]
    heads = (start, w1[0], w2[0], w3[0], first)
    sums = tuple(narrowed(heads[i] * heads[j]) for i, j in PAIRS)
    unused, sums = lax.fori_loop(1, TIME, step, (here, sums), unroll=3)
    sums = tuple(narrowed(start * vector) for vector in heads) + sums
    lane = lax.broadcasted_iota(jnp.int32, (1, 128), 1)
    packed = jnp.zeros((1, 128), f32)
    for place, total in enumerate(sums):
        total = jnp.sum(jnp.sum(total, axis=0, keepdims=True), axis=1, keepdims=True)
        packed = jnp.where(lane == place, total, packed)
    totals[...] = packed


def products(block, table, vectors, wrap):
    scratch = (pltpu.VMEM((TIME, 8, NX), f32),)
    operands = (block, table, *vectors, wrap)
    return call(products_kernel, array(1, 128), "products", scratch, *operands)


def least_squares(gram):
    size = ITERS + 1
    root = [[None] * size for unused in range(size)]
    for i in range(size):
        for j in range(i, size):
            total = gram[i][j]
            for k in range(i):
                total = total - root[k][i] * root[k][j]
            root[i][j] = jnp.sqrt(total) if i == j else total / root[i][i]
    matrix = [[jnp.zeros_like(gram[0][0]) for unused in range(ITERS)] for other in range(size)]
    for column in range(ITERS):
        for row in range(column + 2):
            total = scale * root[row][column + 1]
            if row <= column:
                total = total + (1.0 + shift) * root[row][column]
            matrix[row][column] = total
    target = [root[0][0]] + [jnp.zeros_like(gram[0][0]) for unused in range(ITERS)]
    cosines = []
    sines = []
    for column in range(ITERS):
        for row in range(column):
            upper = matrix[row][column]
            lower = matrix[row + 1][column]
            matrix[row][column] = cosines[row] * upper + sines[row] * lower
            matrix[row + 1][column] = -sines[row] * upper + cosines[row] * lower
        upper = matrix[column][column]
        lower = matrix[column + 1][column]
        radius = jnp.sqrt(upper * upper + lower * lower)
        cosines.append(upper / radius)
        sines.append(lower / radius)
        matrix[column][column] = radius
        target[column + 1] = -sines[column] * target[column]
        target[column] = cosines[column] * target[column]
    factors = [None] * ITERS
    for row in reversed(range(ITERS)):
        total = target[row]
        for other in range(row + 1, ITERS):
            total = total - matrix[row][other] * factors[other]
        factors[row] = total / matrix[row][row]
    return factors


def combine_kernel(totals, z0, z1, z2, z3, out):
    summed = jnp.sum(totals[...], axis=0, keepdims=True)
    size = ITERS + 1
    gram = [[None] * size for unused in range(size)]
    lane = lax.broadcasted_iota(jnp.int32, (1, 128), 1)
    order = [(0, j) for j in range(size)] + PAIRS
    for place, (i, j) in enumerate(order):
        value = jnp.sum(jnp.where(lane == place, summed, 0.0), axis=1, keepdims=True)
        gram[i][j] = value
        gram[j][i] = value
    factors = least_squares(gram)
    for part in range(2):
        value = factors[0] * z0[part]
        for factor, other in zip(factors[1:], (z1, z2, z3)):
            value = value + factor * other[part]
        out[part, 0] = value.T


def combine(totals, fields):
    return call(combine_kernel, array(2, 1, HALF, NY), "combine", (), totals, *fields)


def exchange(value):
    return lax.all_to_all(value, TM_SPACE, split_axis=0, concat_axis=0, tiled=True)


def column_modes(first, count):
    order = first + jnp.arange(count, dtype=jnp.int32)
    return 2 * (order % HALF) + order // HALF


def shards(u_init, phase, absorb):
    step = lax.axis_index(TM)
    half = lax.axis_index("space")
    table = jnp.asarray(TABLES)
    own = column_modes(4 * (2 * step + half), 4)
    other = column_modes(4 * (2 * (step ^ 2) + 1 - half), 4)
    turns = jnp.concatenate([own, other])[:, None] * jnp.arange(NY, dtype=jnp.int32)[None, :] % NY
    angle = turns.astype(f32) * (2.0 * math.pi / NY)
    trig = jnp.concatenate([jnp.cos(angle), jnp.sin(angle)])
    mine, theirs = columns_of(u_init, phase, absorb, trig)
    theirs = lax.ppermute(theirs, ("tm_2", "space"), [(0, 3), (1, 2), (2, 1), (3, 0)])
    block = jnp.where(
        half == 0, jnp.stack([mine, theirs], axis=1), jnp.stack([theirs, mine], axis=1)
    ).reshape(4, 8, HALF)
    own = own.astype(f32)
    rows = jnp.arange(HALF, dtype=jnp.int32)
    rows = jnp.concatenate([2 * rows, 2 * rows + 1]).astype(f32)
    symbol_y = 4.0 * jnp.sin(own * (math.pi / NY)) ** 2
    symbol_x = 4.0 * jnp.sin(rows * (math.pi / NX)) ** 2
    tangent = (0.5 * tau) * (jnp.concatenate([symbol_y, symbol_y])[:, None] + symbol_x[None, :])
    damping = turned(phase, absorb)
    block, damping = lax.optimization_barrier((block, damping))

    vector, wrap, sent, powers = opening(block, tangent, table)
    vectors = [vector]
    found = []
    for column in range(ITERS):
        field, sent = on_cells(exchange(sent), damping, table)
        found.append(field)
        arrived = exchange(sent)
        if column + 1 < ITERS:
            vector, wrap, sent = on_modes(
                arrived, tangent, table, powers, vectors[-1], wrap, column == 0
            )
            vectors.append(vector)
    totals = products(arrived, table, vectors, wrap)
    return combine(exchange(jnp.broadcast_to(totals, (DEVICES, 128))), found)


def solution(mesh):
    torus = Mesh(
        mesh.devices.reshape(4, 4, 2, 2, mesh.shape["space"]),
        ("tm_0", "tm_1", "tm_2", "tm_3", "space"),
    )
    placed = (P(None, "space", None), P("space", None), P("space", None))
    return jax.shard_map(
        shards, mesh=torus, in_specs=placed, out_specs=P(None, TM, "space", None), check_vma=False
    )
```

```python
import math

import jax
import jax.numpy as jnp
import numpy as np
from jax import lax
from jax.experimental import pallas as pl
from jax.experimental.pallas import tpu as pltpu
from jax.sharding import Mesh
from jax.sharding import PartitionSpec as P

NX = 512
NY = 512
HALF = 256
LANES = 128
TIME = 64
ITERS = 4
DEVICES = 128
TM = ("tm_0", "tm_1", "tm_2", "tm_3")
TM_SPACE = ("tm_0", "tm_1", "tm_2", "tm_3", "space")

tau = 400.0
alpha = 0.4
shift = alpha * alpha / (1.0 - alpha * alpha)
scale = alpha / (1.0 - alpha * alpha)
f32 = jnp.float32
bf16 = jnp.bfloat16


def dft_tables():
    mode = np.arange(HALF)[:, None]
    cell = np.arange(HALF)[None, :]
    stack = []
    for frequency, transposed in ((2 * mode, False), (2 * mode + 1, False), (2 * mode + 1, True)):
        angle = 2.0 * np.pi * ((frequency * cell) % NX) / NX
        parts = [np.cos(angle), np.sin(angle)]
        stack.append(np.concatenate([part.T if transposed else part for part in parts]))
    exact = np.stack(stack)
    high = exact.astype(bf16)
    low = (exact - high.astype(np.float64)).astype(bf16)
    return np.stack([high, low])


TABLES = dft_tables()
EVEN, ODD, ODD_T = 0, 1, 2


def halves(value):
    high = value.astype(bf16)
    return high, (value - high.astype(f32)).astype(bf16)


def dot(left, right):
    return jnp.dot(left, right, preferred_element_type=f32)


def dot_last(left, right):
    return lax.dot_general(left, right, (((1,), (1,)), ((), ())), preferred_element_type=f32)


def table_times(table, which, value):
    high, low = halves(value)
    return dot(table[0, which], high) + dot(table[1, which], high) + dot(table[0, which], low)


def times_table(value, table, which):
    high, low = halves(value)
    return dot(high, table[0, which]) + dot(high, table[1, which]) + dot(low, table[0, which])


def call(body, out_shape, name, scratch, *operands, copied=0):
    inside = pl.BlockSpec(memory_space=pltpu.VMEM)
    return pl.pallas_call(
        body,
        out_shape=out_shape,
        in_specs=[pl.BlockSpec(memory_space=pltpu.HBM)] * copied + [inside] * (len(operands) - copied),
        out_specs=jax.tree.map(lambda unused: inside, out_shape),
        scratch_shapes=scratch,
        compiler_params=pltpu.CompilerParams(vmem_limit_bytes=24 << 20),
        name=name,
    )(*operands)


def array(*shape):
    return jax.ShapeDtypeStruct(shape, f32)


def upper_rows(shape):
    return lax.broadcasted_iota(jnp.int32, shape, len(shape) - 2) < 4


def swapped(value):
    return pltpu.roll(value, 4, value.ndim - 2)


def signs(shape, upper, lower):
    return jnp.where(upper_rows(shape), f32(upper), f32(lower))


def split_parts(block):
    pair = block.reshape(32, 2, 8, LANES)
    first, second = pair[:, 0], pair[:, 1]
    upper = upper_rows((1, 8, 1))
    real = jnp.where(upper, first, swapped(second))
    imag = jnp.where(upper, swapped(first), second)
    return real.reshape(HALF, LANES), imag.reshape(HALF, LANES)


def merge_parts(real, imag):
    real = real.reshape(32, 8, LANES)
    imag = imag.reshape(32, 8, LANES)
    upper = upper_rows((1, 8, 1))
    first = jnp.where(upper, real, swapped(imag))
    second = jnp.where(upper, swapped(real), imag)
    return jnp.stack([first, second], axis=1).reshape(64, 8, LANES)


def cells_kernel(arrived, damping, table, field, sent):
    def inverse(part, which, lanes):
        real, imag = split_parts(arrived[pl.ds(part * 64, 64), :, lanes])
        product = table_times(table, which, jnp.concatenate([real, imag], axis=1))
        top, bottom = product[:HALF], product[HALF:]
        return top[:, :LANES] - bottom[:, LANES:], top[:, LANES:] + bottom[:, :LANES]

    def forward(part, which, value, lanes):
        product = table_times(table, which, value)
        top, bottom = product[:HALF], product[HALF:]
        sent[pl.ds(part * 64, 64), :, lanes] = merge_parts(
            top[:, :LANES] + bottom[:, LANES:], top[:, LANES:] - bottom[:, :LANES]
        )

    ranges = [pl.ds(start, LANES) for start in range(0, HALF, LANES)]
    waves = [(inverse(0, EVEN, lanes), inverse(1, ODD_T, lanes)) for lanes in ranges]
    for lanes, (even, odd) in zip(ranges, waves):
        damped = []
        for place, sign in enumerate((1.0, -1.0)):
            rows = pl.ds(place * HALF, HALF)
            real = even[0] + sign * odd[0]
            imag = even[1] + sign * odd[1]
            field[0, rows, lanes] = real
            field[1, rows, lanes] = imag
            absorb = damping[0, rows, lanes]
            phase = damping[1, rows, lanes]
            damped.append(
                jnp.concatenate([absorb * real - phase * imag, absorb * imag + phase * real], axis=1)
            )
        forward(0, EVEN, damped[0] + damped[1], lanes)
        forward(1, ODD, damped[0] - damped[1], lanes)


def on_cells(arrived, damping, table):
    shapes = (array(2, NY, HALF), array(DEVICES, 8, HALF))
    return call(cells_kernel, shapes, "cells", (), arrived, damping, table)


def product_of(real, signed_imag, value):
    return real * value + signed_imag * swapped(value)


def rotation(angle_tangent):
    side = signs((8, NX), -1.0, 1.0)
    inverse = 1.0 / (1.0 + angle_tangent * angle_tangent)
    return (
        (1.0 - angle_tangent * angle_tangent) * inverse,
        -2.0 * angle_tangent * inverse * side,
        inverse,
        -angle_tangent * inverse * side,
    )


def multiplied(left, right):
    return left[0] * right[0] - left[1] * right[1], left[0] * right[1] + left[1] * right[0]


PARTS = ((EVEN, EVEN, 1.0, pl.ds(0, HALF)), (ODD_T, ODD, -1.0, pl.ds(HALF, HALF)))


def rows_forward(block, count, table, into):
    pair = block.reshape(count, 2, 8, HALF)
    side = signs((1, 8, 1), 1.0, -1.0)
    for which, unused, sign, lanes in PARTS:
        value = pair[:, 0] + sign * pair[:, 1]
        value = jnp.concatenate([value, side * swapped(value)], axis=2).reshape(8 * count, NX)
        into[:, :, lanes] = times_table(value, table, which).reshape(count, 8, HALF)


def row_half(modes, table, which, lanes):
    side = signs((1, 8, 1), -1.0, 1.0)
    value = modes[:, :, lanes]
    value = jnp.concatenate([value, side * swapped(value)], axis=2).reshape(TIME * 8, NX)
    return times_table(value, table, which).reshape(TIME, 8, HALF)


def joined(even, odd, sent):
    sent[...] = jnp.stack([even + odd, even - odd], axis=1).reshape(DEVICES, 8, HALF)


def signed_power(turn, count):
    side = signs((8, NX), -1.0, 1.0)
    real, imag = turn[0], turn[1] * side
    for unused in range(count):
        real, imag = real * real - imag * imag, 2.0 * real * imag
    return real, imag, side


def closing(turn):
    real, imag, side = signed_power(turn, 6)
    real, imag = alpha * real, alpha * imag
    rest = 1.0 - real
    inverse = 1.0 / (rest * rest + imag * imag)
    return (real * rest - imag * imag) * inverse, (imag * rest + real * imag) * inverse * side


NORMAL = 1.0 / (NX * NY)


def fetched(sources, targets, arrivals):
    pieces = []
    for source, target in zip(sources, targets):
        for start in range(0, HALF, 64):
            if len(source.shape) == 3:
                pieces += [(source.at[c, pl.ds(start, 64)], target.at[c, pl.ds(start, 64)]) for c in range(2)]
            else:
                pieces.append((source.at[pl.ds(start, 64)], target.at[pl.ds(start, 64)]))
    copies = [
        pltpu.make_async_copy(source, target, arrivals.at[place])
        for place, (source, target) in enumerate(pieces)
    ]
    for copy in copies:
        copy.start()
    for copy in copies:
        copy.wait()


def columns_kernel(far_field, far_phase, far_absorb, trig, mine, theirs, field, phase, absorb, arrivals):
    fetched((far_field, far_phase, far_absorb), (field, phase, absorb), arrivals)
    real, imag = field[0], field[1]
    damped_real = 0.5 * (absorb[...] * real - phase[...] * imag)
    damped_imag = 0.5 * (absorb[...] * imag + phase[...] * real)
    high, low = halves(jnp.concatenate([real, imag, damped_real, damped_imag], axis=0))
    trig_high, trig_low = halves(trig[...])
    product = dot_last(trig_high, high) + dot_last(trig_low, high) + dot_last(trig_high, low)
    upper = upper_rows((8, 1))
    for place in range(2):
        start = 2 * place * HALF
        first = product[:, start : start + HALF]
        second = product[:, start + HALF : start + 2 * HALF]
        real = first[:8] + second[8:]
        imag = second[:8] - first[8:]
        mine[place] = jnp.where(upper, real, swapped(imag))
        theirs[place] = jnp.where(upper, swapped(real), imag)


def columns_of(field, phase, absorb, trig):
    far = [pltpu.with_memory_space_constraint(value, pltpu.HBM) for value in (field, phase, absorb)]
    operands = (*far, trig)
    scratch = (
        pltpu.VMEM((2, HALF, NY), f32),
        pltpu.VMEM((HALF, NY), f32),
        pltpu.VMEM((HALF, NY), f32),
        pltpu.SemaphoreType.DMA((16,)),
    )
    shapes = (array(2, 8, HALF), array(2, 8, HALF))
    return call(columns_kernel, shapes, "columns", scratch, *operands, copied=3)


def turning_kernel(phase, absorb, damping):
    damping[0] = (0.5 / scale) * absorb[...].T
    damping[1] = (0.5 / scale) * phase[...].T


def turned(phase, absorb):
    return call(turning_kernel, array(2, NY, HALF), "turning", (), phase, absorb)


def opening_kernel(block, tangent, table, vector, offset, sent, powers, spectrum, modes):
    rows_forward(block[...], 2, table, spectrum)
    slope = tangent[...]
    turn_real, turn_imag, gain_real, gain_imag = rotation(slope)
    side = signs((8, NX), -1.0, 1.0)
    wave, damped = spectrum[0], spectrum[1]
    vector[...] = product_of(1.0, -slope * side, wave) - damped
    value = product_of(turn_real, turn_imag, wave) - product_of(gain_real, gain_imag, damped)
    wrap = product_of(*closing((turn_real, turn_imag)), value)
    offset[...] = product_of(1.0, slope * side, wrap)
    start = NORMAL * (wrap + value)

    def step(n, power):
        real, imag = power
        powers[n, 0] = real
        powers[n, 1] = imag
        modes[n] = product_of(real, imag, start)
        return real * turn_real - imag * turn_imag, real * turn_imag + imag * turn_real

    one = jnp.ones((8, NX), f32)
    lax.fori_loop(0, TIME, step, (one, jnp.zeros((8, NX), f32)), unroll=4)
    joined(*[row_half(modes, table, which, lanes) for unused, which, sign, lanes in PARTS], sent)


def opening(block, tangent, table):
    shapes = (
        array(8, NX),
        array(8, NX),
        array(DEVICES, 8, HALF),
        array(TIME, 2, 8, NX),
    )
    scratch = (pltpu.VMEM((2, 8, NX), f32), pltpu.VMEM((TIME, 8, NX), f32))
    return call(opening_kernel, shapes, "opening", scratch, block, tangent, table)


def modes_kernel_of(first):
    def body(block, tangent, table, powers, earlier, wrap_in, vector, wrap_out, sent, modes, sums):
        rows_forward(block[...], TIME, table, modes)
        slope = tangent[...]
        turn_real, turn_imag, gain_real, gain_imag = rotation(slope)
        start = (1.0 / scale) * wrap_in[...]
        if first:
            start = start - alpha * earlier[...]
        closed = closing((turn_real, turn_imag))
        gain_real, gain_imag = NORMAL * gain_real, NORMAL * gain_imag
        wraps = []
        for part in range(2):
            lanes = PARTS[part][3]
            before = start[:, part * HALF : (part + 1) * HALF]
            total = jnp.zeros((8, HALF), f32)
            for n in range(TIME):
                here = modes[n, :, lanes]
                value = here + before
                before = here
                if not first:
                    value = value - alpha * earlier[n, :, lanes]
                vector[n, :, lanes] = value
                total = total + product_of(powers[n, 0, :, lanes], -powers[n, 1, :, lanes], value)
                sums[n, :, lanes] = total
            columns = slice(part * HALF, (part + 1) * HALF)
            wraps.append(product_of(closed[0][:, columns], closed[1][:, columns], total))
            wrap_out[:, lanes] = wraps[part]
        found = []
        for part, (unused, which, sign, lanes) in enumerate(PARTS):
            columns = slice(part * HALF, (part + 1) * HALF)
            gain = (gain_real[:, columns], gain_imag[:, columns])
            for n in range(TIME):
                value = product_of(*gain, wraps[part] + sums[n, :, lanes])
                modes[n, :, lanes] = product_of(
                    powers[n, 0, :, lanes], powers[n, 1, :, lanes], value
                )
            found.append(row_half(modes, table, which, lanes))
        joined(*found, sent)

    return body


def on_modes(block, tangent, table, powers, earlier, wrap, first):
    shapes = (array(TIME, 8, NX), array(8, NX), array(DEVICES, 8, HALF))
    scratch = (pltpu.VMEM((TIME, 8, NX), f32), pltpu.VMEM((TIME, 8, NX), f32))
    body = modes_kernel_of(first)
    operands = (block, tangent, table, powers, earlier, wrap)
    return call(body, shapes, "modes", scratch, *operands)


PAIRS = [(i, j) for i in range(1, ITERS + 1) for j in range(i, ITERS + 1)]


def products_kernel(block, table, w0, w1, w2, w3, wrap, totals, spectrum):
    rows_forward(block[...], TIME, table, spectrum)

    def narrowed(value):
        return value[:, 0:128] + value[:, 128:256] + value[:, 256:384] + value[:, 384:512]

    def step(n, carry):
        before, sums = carry
        here = spectrum[n]
        value = here + before - alpha * w3[n]
        vectors = (None, w1[n], w2[n], w3[n], value)
        sums = tuple(
            total + narrowed(vectors[i] * vectors[j]) for total, (i, j) in zip(sums, PAIRS)
        )
        return here, sums

    start = w0[...]
    here = spectrum[0]
    first = here + (1.0 / scale) * wrap[...] - alpha * w3[0]
    heads = (start, w1[0], w2[0], w3[0], first)
    sums = tuple(narrowed(heads[i] * heads[j]) for i, j in PAIRS)
    unused, sums = lax.fori_loop(1, TIME, step, (here, sums), unroll=3)
    sums = tuple(narrowed(start * vector) for vector in heads) + sums
    lane = lax.broadcasted_iota(jnp.int32, (1, 128), 1)
    packed = jnp.zeros((1, 128), f32)
    for place, total in enumerate(sums):
        total = jnp.sum(jnp.sum(total, axis=0, keepdims=True), axis=1, keepdims=True)
        packed = jnp.where(lane == place, total, packed)
    totals[...] = packed


def products(block, table, vectors, wrap):
    scratch = (pltpu.VMEM((TIME, 8, NX), f32),)
    operands = (block, table, *vectors, wrap)
    return call(products_kernel, array(1, 128), "products", scratch, *operands)


def least_squares(gram):
    size = ITERS + 1
    root = [[None] * size for unused in range(size)]
    for i in range(size):
        for j in range(i, size):
            total = gram[i][j]
            for k in range(i):
                total = total - root[k][i] * root[k][j]
            root[i][j] = jnp.sqrt(total) if i == j else total / root[i][i]
    matrix = [[jnp.zeros_like(gram[0][0]) for unused in range(ITERS)] for other in range(size)]
    for column in range(ITERS):
        for row in range(column + 2):
            total = scale * root[row][column + 1]
            if row <= column:
                total = total + (1.0 + shift) * root[row][column]
            matrix[row][column] = total
    target = [root[0][0]] + [jnp.zeros_like(gram[0][0]) for unused in range(ITERS)]
    cosines = []
    sines = []
    for column in range(ITERS):
        for row in range(column):
            upper = matrix[row][column]
            lower = matrix[row + 1][column]
            matrix[row][column] = cosines[row] * upper + sines[row] * lower
            matrix[row + 1][column] = -sines[row] * upper + cosines[row] * lower
        upper = matrix[column][column]
        lower = matrix[column + 1][column]
        radius = jnp.sqrt(upper * upper + lower * lower)
        cosines.append(upper / radius)
        sines.append(lower / radius)
        matrix[column][column] = radius
        target[column + 1] = -sines[column] * target[column]
        target[column] = cosines[column] * target[column]
    factors = [None] * ITERS
    for row in reversed(range(ITERS)):
        total = target[row]
        for other in range(row + 1, ITERS):
            total = total - matrix[row][other] * factors[other]
        factors[row] = total / matrix[row][row]
    return factors


def combine_kernel(totals, z0, z1, z2, z3, out):
    summed = jnp.sum(totals[...], axis=0, keepdims=True)
    size = ITERS + 1
    gram = [[None] * size for unused in range(size)]
    lane = lax.broadcasted_iota(jnp.int32, (1, 128), 1)
    order = [(0, j) for j in range(size)] + PAIRS
    for place, (i, j) in enumerate(order):
        value = jnp.sum(jnp.where(lane == place, summed, 0.0), axis=1, keepdims=True)
        gram[i][j] = value
        gram[j][i] = value
    factors = least_squares(gram)
    for part in range(2):
        value = factors[0] * z0[part]
        for factor, other in zip(factors[1:], (z1, z2, z3)):
            value = value + factor * other[part]
        out[part, 0] = value.T


def combine(totals, fields):
    return call(combine_kernel, array(2, 1, HALF, NY), "combine", (), totals, *fields)


def exchange(value):
    return lax.all_to_all(value, TM_SPACE, split_axis=0, concat_axis=0, tiled=True)


def column_modes(first, count):
    order = first + jnp.arange(count, dtype=jnp.int32)
    return 2 * (order % HALF) + order // HALF


def shards(u_init, phase, absorb):
    step = lax.axis_index(TM)
    half = lax.axis_index("space")
    table = jnp.asarray(TABLES)
    own = column_modes(4 * (2 * step + half), 4)
    other = column_modes(4 * (2 * (step ^ 2) + 1 - half), 4)
    turns = jnp.concatenate([own, other])[:, None] * jnp.arange(NY, dtype=jnp.int32)[None, :] % NY
    angle = turns.astype(f32) * (2.0 * math.pi / NY)
    trig = jnp.concatenate([jnp.cos(angle), jnp.sin(angle)])
    mine, theirs = columns_of(u_init, phase, absorb, trig)
    theirs = lax.ppermute(theirs, ("tm_2", "space"), [(0, 3), (1, 2), (2, 1), (3, 0)])
    block = jnp.where(
        half == 0, jnp.stack([mine, theirs], axis=1), jnp.stack([theirs, mine], axis=1)
    ).reshape(4, 8, HALF)
    own = own.astype(f32)
    rows = jnp.arange(HALF, dtype=jnp.int32)
    rows = jnp.concatenate([2 * rows, 2 * rows + 1]).astype(f32)
    symbol_y = 4.0 * jnp.sin(own * (math.pi / NY)) ** 2
    symbol_x = 4.0 * jnp.sin(rows * (math.pi / NX)) ** 2
    tangent = (0.5 * tau) * (jnp.concatenate([symbol_y, symbol_y])[:, None] + symbol_x[None, :])
    damping = turned(phase, absorb)
    block, damping = lax.optimization_barrier((block, damping))

    vector, wrap, sent, powers = opening(block, tangent, table)
    vectors = [vector]
    found = []
    for column in range(ITERS):
        field, sent = on_cells(exchange(sent), damping, table)
        found.append(field)
        arrived = exchange(sent)
        if column + 1 < ITERS:
            vector, wrap, sent = on_modes(
                arrived, tangent, table, powers, vectors[-1], wrap, column == 0
            )
            vectors.append(vector)
    totals = products(arrived, table, vectors, wrap)
    return combine(exchange(jnp.broadcast_to(totals, (DEVICES, 128))), found)


def solution(mesh):
    torus = Mesh(
        mesh.devices.reshape(4, 4, 2, 2, mesh.shape["space"]),
        ("tm_0", "tm_1", "tm_2", "tm_3", "space"),
    )
    placed = (P(None, "space", None), P("space", None), P("space", None))
    return jax.shard_map(
        shards, mesh=torus, in_specs=placed, out_specs=P(None, TM, "space", None), check_vma=False
    )
```

```python
import math

import jax
import jax.numpy as jnp
import numpy as np
from jax import lax
from jax.experimental import pallas as pl
from jax.experimental.pallas import tpu as pltpu
from jax.sharding import Mesh
from jax.sharding import PartitionSpec as P

NX = 512
NY = 512
HALF = 256
LANES = 128
TIME = 64
ITERS = 4
DEVICES = 128
TM = ("tm_0", "tm_1", "tm_2", "tm_3")
TM_SPACE = ("tm_0", "tm_1", "tm_2", "tm_3", "space")

tau = 400.0
alpha = 0.4
shift = alpha * alpha / (1.0 - alpha * alpha)
scale = alpha / (1.0 - alpha * alpha)
f32 = jnp.float32
bf16 = jnp.bfloat16


def dft_tables():
    mode = np.arange(HALF)[:, None]
    cell = np.arange(HALF)[None, :]
    stack = []
    for frequency, transposed in ((2 * mode, False), (2 * mode + 1, False), (2 * mode + 1, True)):
        angle = 2.0 * np.pi * ((frequency * cell) % NX) / NX
        parts = [np.cos(angle), np.sin(angle)]
        stack.append(np.concatenate([part.T if transposed else part for part in parts]))
    exact = np.stack(stack)
    high = exact.astype(bf16)
    low = (exact - high.astype(np.float64)).astype(bf16)
    return np.stack([high, low])


TABLES = dft_tables()
EVEN, ODD, ODD_T = 0, 1, 2


def halves(value):
    high = value.astype(bf16)
    return high, (value - high.astype(f32)).astype(bf16)


def dot(left, right):
    return jnp.dot(left, right, preferred_element_type=f32)


def dot_last(left, right):
    return lax.dot_general(left, right, (((1,), (1,)), ((), ())), preferred_element_type=f32)


def table_times(table, which, value):
    high, low = halves(value)
    return dot(table[0, which], high) + dot(table[1, which], high) + dot(table[0, which], low)


def times_table(value, table, which):
    high, low = halves(value)
    return dot(high, table[0, which]) + dot(high, table[1, which]) + dot(low, table[0, which])


def call(body, out_shape, name, scratch, *operands, copied=0):
    inside = pl.BlockSpec(memory_space=pltpu.VMEM)
    return pl.pallas_call(
        body,
        out_shape=out_shape,
        in_specs=[pl.BlockSpec(memory_space=pltpu.HBM)] * copied + [inside] * (len(operands) - copied),
        out_specs=jax.tree.map(lambda unused: inside, out_shape),
        scratch_shapes=scratch,
        compiler_params=pltpu.CompilerParams(vmem_limit_bytes=24 << 20),
        name=name,
    )(*operands)


def array(*shape):
    return jax.ShapeDtypeStruct(shape, f32)


def upper_rows(shape):
    return lax.broadcasted_iota(jnp.int32, shape, len(shape) - 2) < 4


def swapped(value):
    return pltpu.roll(value, 4, value.ndim - 2)


def signs(shape, upper, lower):
    return jnp.where(upper_rows(shape), f32(upper), f32(lower))


def split_parts(block):
    pair = block.reshape(32, 2, 8, LANES)
    first, second = pair[:, 0], pair[:, 1]
    upper = upper_rows((1, 8, 1))
    real = jnp.where(upper, first, swapped(second))
    imag = jnp.where(upper, swapped(first), second)
    return real.reshape(HALF, LANES), imag.reshape(HALF, LANES)


def merge_parts(real, imag):
    real = real.reshape(32, 8, LANES)
    imag = imag.reshape(32, 8, LANES)
    upper = upper_rows((1, 8, 1))
    first = jnp.where(upper, real, swapped(imag))
    second = jnp.where(upper, swapped(real), imag)
    return jnp.stack([first, second], axis=1).reshape(64, 8, LANES)


def cells_kernel(arrived, damping, table, field, sent):
    def inverse(part, which, lanes):
        real, imag = split_parts(arrived[pl.ds(part * 64, 64), :, lanes])
        product = table_times(table, which, jnp.concatenate([real, imag], axis=1))
        top, bottom = product[:HALF], product[HALF:]
        return top[:, :LANES] - bottom[:, LANES:], top[:, LANES:] + bottom[:, :LANES]

    def forward(part, which, value, lanes):
        product = table_times(table, which, value)
        top, bottom = product[:HALF], product[HALF:]
        sent[pl.ds(part * 64, 64), :, lanes] = merge_parts(
            top[:, :LANES] + bottom[:, LANES:], top[:, LANES:] - bottom[:, :LANES]
        )

    ranges = [pl.ds(start, LANES) for start in range(0, HALF, LANES)]
    waves = [(inverse(0, EVEN, lanes), inverse(1, ODD_T, lanes)) for lanes in ranges]
    for lanes, (even, odd) in zip(ranges, waves):
        damped = []
        for place, sign in enumerate((1.0, -1.0)):
            rows = pl.ds(place * HALF, HALF)
            real = even[0] + sign * odd[0]
            imag = even[1] + sign * odd[1]
            field[0, rows, lanes] = real
            field[1, rows, lanes] = imag
            absorb = damping[0, rows, lanes]
            phase = damping[1, rows, lanes]
            damped.append(
                jnp.concatenate([absorb * real - phase * imag, absorb * imag + phase * real], axis=1)
            )
        forward(0, EVEN, damped[0] + damped[1], lanes)
        forward(1, ODD, damped[0] - damped[1], lanes)


def on_cells(arrived, damping, table):
    shapes = (array(2, NY, HALF), array(DEVICES, 8, HALF))
    return call(cells_kernel, shapes, "cells", (), arrived, damping, table)


def product_of(real, signed_imag, value):
    return real * value + signed_imag * swapped(value)


def rotation(angle_tangent):
    side = signs((8, NX), -1.0, 1.0)
    inverse = 1.0 / (1.0 + angle_tangent * angle_tangent)
    return (
        (1.0 - angle_tangent * angle_tangent) * inverse,
        -2.0 * angle_tangent * inverse * side,
        inverse,
        -angle_tangent * inverse * side,
    )


def multiplied(left, right):
    return left[0] * right[0] - left[1] * right[1], left[0] * right[1] + left[1] * right[0]


PARTS = ((EVEN, EVEN, 1.0, pl.ds(0, HALF)), (ODD_T, ODD, -1.0, pl.ds(HALF, HALF)))


def rows_forward(block, count, table, into):
    pair = block.reshape(count, 2, 8, HALF)
    side = signs((1, 8, 1), 1.0, -1.0)
    for which, unused, sign, lanes in PARTS:
        value = pair[:, 0] + sign * pair[:, 1]
        value = jnp.concatenate([value, side * swapped(value)], axis=2).reshape(8 * count, NX)
        into[:, :, lanes] = times_table(value, table, which).reshape(count, 8, HALF)


def row_half(modes, table, which, lanes):
    side = signs((1, 8, 1), -1.0, 1.0)
    value = modes[:, :, lanes]
    value = jnp.concatenate([value, side * swapped(value)], axis=2).reshape(TIME * 8, NX)
    return times_table(value, table, which).reshape(TIME, 8, HALF)


def joined(even, odd, sent):
    sent[...] = jnp.stack([even + odd, even - odd], axis=1).reshape(DEVICES, 8, HALF)


def signed_power(turn, count):
    side = signs((8, NX), -1.0, 1.0)
    real, imag = turn[0], turn[1] * side
    for unused in range(count):
        real, imag = real * real - imag * imag, 2.0 * real * imag
    return real, imag, side


def closing(turn):
    real, imag, side = signed_power(turn, 6)
    real, imag = alpha * real, alpha * imag
    rest = 1.0 - real
    inverse = 1.0 / (rest * rest + imag * imag)
    return (real * rest - imag * imag) * inverse, (imag * rest + real * imag) * inverse * side


NORMAL = 1.0 / (NX * NY)


def columns_kernel(
    far_field, far_phase, far_absorb, trig, mine, theirs, field, phase, absorb, arrivals
):
    pairs = ((far_field, field), (far_phase, phase), (far_absorb, absorb))
    copies = [
        pltpu.make_async_copy(source, target, arrivals.at[place])
        for place, (source, target) in enumerate(pairs)
    ]
    for copy in copies:
        copy.start()
    trig_high, trig_low = halves(trig[...])

    def transformed(*values):
        high, low = halves(jnp.concatenate(values, axis=0))
        return dot_last(trig_high, high) + dot_last(trig_low, high) + dot_last(trig_high, low)

    copies[0].wait()
    real, imag = field[0], field[1]
    start_product = transformed(real, imag)
    copies[1].wait()
    copies[2].wait()
    damped_product = transformed(
        0.5 * (absorb[...] * real - phase[...] * imag),
        0.5 * (absorb[...] * imag + phase[...] * real),
    )
    upper = upper_rows((8, 1))
    for place, product in enumerate((start_product, damped_product)):
        first, second = product[:, :HALF], product[:, HALF:]
        real = first[:8] + second[8:]
        imag = second[:8] - first[8:]
        mine[place] = jnp.where(upper, real, swapped(imag))
        theirs[place] = jnp.where(upper, swapped(real), imag)


def columns_of(field, phase, absorb, trig):
    far = [pltpu.with_memory_space_constraint(value, pltpu.HBM) for value in (field, phase, absorb)]
    operands = (*far, trig)
    scratch = (
        pltpu.VMEM((2, HALF, NY), f32),
        pltpu.VMEM((HALF, NY), f32),
        pltpu.VMEM((HALF, NY), f32),
        pltpu.SemaphoreType.DMA((3,)),
    )
    shapes = (array(2, 8, HALF), array(2, 8, HALF))
    return call(columns_kernel, shapes, "columns", scratch, *operands, copied=3)


def turning_kernel(phase, absorb, damping):
    damping[0] = (0.5 / scale) * absorb[...].T
    damping[1] = (0.5 / scale) * phase[...].T


def turned(phase, absorb):
    return call(turning_kernel, array(2, NY, HALF), "turning", (), phase, absorb)


def opening_kernel(block, tangent, table, vector, offset, sent, powers, spectrum, modes):
    rows_forward(block[...], 2, table, spectrum)
    slope = tangent[...]
    turn_real, turn_imag, gain_real, gain_imag = rotation(slope)
    side = signs((8, NX), -1.0, 1.0)
    wave, damped = spectrum[0], spectrum[1]
    vector[...] = product_of(1.0, -slope * side, wave) - damped
    value = product_of(turn_real, turn_imag, wave) - product_of(gain_real, gain_imag, damped)
    wrap = product_of(*closing((turn_real, turn_imag)), value)
    offset[...] = product_of(1.0, slope * side, wrap)
    start = NORMAL * (wrap + value)

    found = []
    for part, (unused, which, sign, lanes) in enumerate(PARTS):
        columns = slice(part * HALF, (part + 1) * HALF)
        turn = turn_real[:, columns], turn_imag[:, columns]
        real, imag = jnp.ones((8, HALF), f32), jnp.zeros((8, HALF), f32)
        for n in range(TIME):
            powers[n, 0, :, lanes] = real
            powers[n, 1, :, lanes] = imag
            modes[n, :, lanes] = product_of(real, imag, start[:, columns])
            real, imag = real * turn[0] - imag * turn[1], real * turn[1] + imag * turn[0]
        found.append(row_half(modes, table, which, lanes))
    joined(*found, sent)


def opening(block, tangent, table):
    shapes = (
        array(8, NX),
        array(8, NX),
        array(DEVICES, 8, HALF),
        array(TIME, 2, 8, NX),
    )
    scratch = (pltpu.VMEM((2, 8, NX), f32), pltpu.VMEM((TIME, 8, NX), f32))
    return call(opening_kernel, shapes, "opening", scratch, block, tangent, table)


def modes_kernel_of(first):
    def body(block, tangent, table, powers, earlier, wrap_in, vector, wrap_out, sent, modes, sums):
        rows_forward(block[...], TIME, table, modes)
        slope = tangent[...]
        turn_real, turn_imag, gain_real, gain_imag = rotation(slope)
        start = (1.0 / scale) * wrap_in[...]
        if first:
            start = start - alpha * earlier[...]
        closed = closing((turn_real, turn_imag))
        gain_real, gain_imag = NORMAL * gain_real, NORMAL * gain_imag
        wraps = []
        for part in range(2):
            lanes = PARTS[part][3]
            before = start[:, part * HALF : (part + 1) * HALF]
            total = jnp.zeros((8, HALF), f32)
            for n in range(TIME):
                here = modes[n, :, lanes]
                value = here + before
                before = here
                if not first:
                    value = value - alpha * earlier[n, :, lanes]
                vector[n, :, lanes] = value
                total = total + product_of(powers[n, 0, :, lanes], -powers[n, 1, :, lanes], value)
                sums[n, :, lanes] = total
            columns = slice(part * HALF, (part + 1) * HALF)
            wraps.append(product_of(closed[0][:, columns], closed[1][:, columns], total))
            wrap_out[:, lanes] = wraps[part]
        found = []
        for part, (unused, which, sign, lanes) in enumerate(PARTS):
            columns = slice(part * HALF, (part + 1) * HALF)
            gain = (gain_real[:, columns], gain_imag[:, columns])
            for n in range(TIME):
                value = product_of(*gain, wraps[part] + sums[n, :, lanes])
                modes[n, :, lanes] = product_of(
                    powers[n, 0, :, lanes], powers[n, 1, :, lanes], value
                )
            found.append(row_half(modes, table, which, lanes))
        joined(*found, sent)

    return body


def on_modes(block, tangent, table, powers, earlier, wrap, first):
    shapes = (array(TIME, 8, NX), array(8, NX), array(DEVICES, 8, HALF))
    scratch = (pltpu.VMEM((TIME, 8, NX), f32), pltpu.VMEM((TIME, 8, NX), f32))
    body = modes_kernel_of(first)
    operands = (block, tangent, table, powers, earlier, wrap)
    return call(body, shapes, "modes", scratch, *operands)


PAIRS = [(i, j) for i in range(1, ITERS + 1) for j in range(i, ITERS + 1)]


def products_kernel(block, table, w0, w1, w2, w3, wrap, totals, spectrum):
    rows_forward(block[...], TIME, table, spectrum)

    sums = [None] * (len(PAIRS) + ITERS + 1)
    order = [(0, j) for j in range(ITERS + 1)] + PAIRS

    def add(place, value):
        value = value[:, :LANES] + value[:, LANES:]
        sums[place] = value if sums[place] is None else sums[place] + value

    for part in range(2):
        lanes = PARTS[part][3]
        before = (1.0 / scale) * wrap[:, lanes]
        for n in range(TIME):
            here = spectrum[n, :, lanes]
            vectors = [w[n, :, lanes] for w in (w1, w2, w3)]
            vectors.append(here + before - alpha * vectors[2])
            vectors.insert(0, w0[:, lanes] if n == 0 else None)
            before = here
            for place, (i, j) in enumerate(order):
                if vectors[i] is not None:
                    add(place, vectors[i] * vectors[j])

    lane = lax.broadcasted_iota(jnp.int32, (1, 128), 1)
    packed = jnp.zeros((1, 128), f32)
    for place, total in enumerate(sums):
        total = jnp.sum(jnp.sum(total, axis=0, keepdims=True), axis=1, keepdims=True)
        packed = jnp.where(lane == place, total, packed)
    totals[...] = packed


def products(block, table, vectors, wrap):
    scratch = (pltpu.VMEM((TIME, 8, NX), f32),)
    operands = (block, table, *vectors, wrap)
    return call(products_kernel, array(1, 128), "products", scratch, *operands)


def least_squares(gram):
    size = ITERS + 1
    root = [[None] * size for unused in range(size)]
    for i in range(size):
        for j in range(i, size):
            total = gram[i][j]
            for k in range(i):
                total = total - root[k][i] * root[k][j]
            root[i][j] = jnp.sqrt(total) if i == j else total / root[i][i]
    matrix = [[jnp.zeros_like(gram[0][0]) for unused in range(ITERS)] for other in range(size)]
    for column in range(ITERS):
        for row in range(column + 2):
            total = scale * root[row][column + 1]
            if row <= column:
                total = total + (1.0 + shift) * root[row][column]
            matrix[row][column] = total
    target = [root[0][0]] + [jnp.zeros_like(gram[0][0]) for unused in range(ITERS)]
    cosines = []
    sines = []
    for column in range(ITERS):
        for row in range(column):
            upper = matrix[row][column]
            lower = matrix[row + 1][column]
            matrix[row][column] = cosines[row] * upper + sines[row] * lower
            matrix[row + 1][column] = -sines[row] * upper + cosines[row] * lower
        upper = matrix[column][column]
        lower = matrix[column + 1][column]
        radius = jnp.sqrt(upper * upper + lower * lower)
        cosines.append(upper / radius)
        sines.append(lower / radius)
        matrix[column][column] = radius
        target[column + 1] = -sines[column] * target[column]
        target[column] = cosines[column] * target[column]
    factors = [None] * ITERS
    for row in reversed(range(ITERS)):
        total = target[row]
        for other in range(row + 1, ITERS):
            total = total - matrix[row][other] * factors[other]
        factors[row] = total / matrix[row][row]
    return factors


def combine_kernel(totals, z0, z1, z2, z3, out):
    summed = jnp.sum(totals[...], axis=0, keepdims=True)
    size = ITERS + 1
    gram = [[None] * size for unused in range(size)]
    lane = lax.broadcasted_iota(jnp.int32, (1, 128), 1)
    order = [(0, j) for j in range(size)] + PAIRS
    for place, (i, j) in enumerate(order):
        value = jnp.sum(jnp.where(lane == place, summed, 0.0), axis=1, keepdims=True)
        gram[i][j] = value
        gram[j][i] = value
    factors = least_squares(gram)
    for part in range(2):
        value = factors[0] * z0[part]
        for factor, other in zip(factors[1:], (z1, z2, z3)):
            value = value + factor * other[part]
        out[part, 0] = value.T


def combine(totals, fields):
    return call(combine_kernel, array(2, 1, HALF, NY), "combine", (), totals, *fields)


def exchange(value):
    return lax.all_to_all(value, TM_SPACE, split_axis=0, concat_axis=0, tiled=True)


def column_modes(first, count):
    order = first + jnp.arange(count, dtype=jnp.int32)
    return 2 * (order % HALF) + order // HALF


def shards(u_init, phase, absorb):
    step = lax.axis_index(TM)
    half = lax.axis_index("space")
    table = jnp.asarray(TABLES)
    own = column_modes(4 * (2 * step + half), 4)
    other = column_modes(4 * (2 * (step ^ 2) + 1 - half), 4)
    turns = jnp.concatenate([own, other])[:, None] * jnp.arange(NY, dtype=jnp.int32)[None, :] % NY
    angle = turns.astype(f32) * (2.0 * math.pi / NY)
    trig = jnp.concatenate([jnp.cos(angle), jnp.sin(angle)])
    mine, theirs = columns_of(u_init, phase, absorb, trig)
    theirs = lax.ppermute(theirs, ("tm_2", "space"), [(0, 3), (1, 2), (2, 1), (3, 0)])
    block = jnp.where(
        half == 0, jnp.stack([mine, theirs], axis=1), jnp.stack([theirs, mine], axis=1)
    ).reshape(4, 8, HALF)
    own = own.astype(f32)
    rows = jnp.arange(HALF, dtype=jnp.int32)
    rows = jnp.concatenate([2 * rows, 2 * rows + 1]).astype(f32)
    symbol_y = 4.0 * jnp.sin(own * (math.pi / NY)) ** 2
    symbol_x = 4.0 * jnp.sin(rows * (math.pi / NX)) ** 2
    tangent = (0.5 * tau) * (jnp.concatenate([symbol_y, symbol_y])[:, None] + symbol_x[None, :])
    damping = turned(phase, absorb)
    block, damping = lax.optimization_barrier((block, damping))

    vector, wrap, sent, powers = opening(block, tangent, table)
    vectors = [vector]
    found = []
    for column in range(ITERS):
        field, sent = on_cells(exchange(sent), damping, table)
        found.append(field)
        arrived = exchange(sent)
        if column + 1 < ITERS:
            vector, wrap, sent = on_modes(
                arrived, tangent, table, powers, vectors[-1], wrap, column == 0
            )
            vectors.append(vector)
    totals = products(arrived, table, vectors, wrap)
    return combine(exchange(jnp.broadcast_to(totals, (DEVICES, 128))), found)


def solution(mesh):
    torus = Mesh(
        mesh.devices.reshape(4, 4, 2, 2, mesh.shape["space"]),
        ("tm_0", "tm_1", "tm_2", "tm_3", "space"),
    )
    placed = (P(None, "space", None), P("space", None), P("space", None))
    return jax.shard_map(
        shards, mesh=torus, in_specs=placed, out_specs=P(None, TM, "space", None), check_vma=False
    )
```

```python
import math

import jax
import jax.numpy as jnp
import numpy as np
from jax import lax
from jax.experimental import pallas as pl
from jax.experimental.pallas import tpu as pltpu
from jax.sharding import Mesh
from jax.sharding import PartitionSpec as P

NX = 512
NY = 512
HALF = 256
LANES = 128
TIME = 64
ITERS = 4
DEVICES = 128
TM = ("tm_0", "tm_1", "tm_2", "tm_3")
TM_SPACE = ("tm_0", "tm_1", "tm_2", "tm_3", "space")

tau = 400.0
alpha = 0.4
shift = alpha * alpha / (1.0 - alpha * alpha)
scale = alpha / (1.0 - alpha * alpha)
f32 = jnp.float32
bf16 = jnp.bfloat16


def dft_tables():
    mode = np.arange(HALF)[:, None]
    cell = np.arange(HALF)[None, :]
    stack = []
    for frequency, transposed in ((2 * mode, False), (2 * mode + 1, False), (2 * mode + 1, True)):
        angle = 2.0 * np.pi * ((frequency * cell) % NX) / NX
        parts = [np.cos(angle), np.sin(angle)]
        stack.append(np.concatenate([part.T if transposed else part for part in parts]))
    exact = np.stack(stack)
    high = exact.astype(bf16)
    low = (exact - high.astype(np.float64)).astype(bf16)
    return np.stack([high, low])


TABLES = dft_tables()
EVEN, ODD, ODD_T = 0, 1, 2


def halves(value):
    high = value.astype(bf16)
    return high, (value - high.astype(f32)).astype(bf16)


def dot(left, right):
    return jnp.dot(left, right, preferred_element_type=f32)


def dot_last(left, right):
    return lax.dot_general(left, right, (((1,), (1,)), ((), ())), preferred_element_type=f32)


def table_times(table, which, value):
    high, low = halves(value)
    return dot(table[0, which], high) + dot(table[1, which], high) + dot(table[0, which], low)


def times_table(value, table, which):
    high, low = halves(value)
    return dot(high, table[0, which]) + dot(high, table[1, which]) + dot(low, table[0, which])


def call(body, out_shape, name, scratch, *operands, copied=0):
    inside = pl.BlockSpec(memory_space=pltpu.VMEM)
    return pl.pallas_call(
        body,
        out_shape=out_shape,
        in_specs=[pl.BlockSpec(memory_space=pltpu.HBM)] * copied + [inside] * (len(operands) - copied),
        out_specs=jax.tree.map(lambda unused: inside, out_shape),
        scratch_shapes=scratch,
        compiler_params=pltpu.CompilerParams(vmem_limit_bytes=24 << 20),
        name=name,
    )(*operands)


def array(*shape):
    return jax.ShapeDtypeStruct(shape, f32)


def upper_rows(shape):
    return lax.broadcasted_iota(jnp.int32, shape, len(shape) - 2) < 4


def swapped(value):
    return pltpu.roll(value, 4, value.ndim - 2)


def signs(shape, upper, lower):
    return jnp.where(upper_rows(shape), f32(upper), f32(lower))


def split_parts(block):
    pair = block.reshape(32, 2, 8, LANES)
    first, second = pair[:, 0], pair[:, 1]
    upper = upper_rows((1, 8, 1))
    real = jnp.where(upper, first, swapped(second))
    imag = jnp.where(upper, swapped(first), second)
    return real.reshape(HALF, LANES), imag.reshape(HALF, LANES)


def merge_parts(real, imag):
    real = real.reshape(32, 8, LANES)
    imag = imag.reshape(32, 8, LANES)
    upper = upper_rows((1, 8, 1))
    first = jnp.where(upper, real, swapped(imag))
    second = jnp.where(upper, swapped(real), imag)
    return jnp.stack([first, second], axis=1).reshape(64, 8, LANES)


def cells_kernel(arrived, damping, table, field, sent):
    def inverse(part, which, lanes):
        real, imag = split_parts(arrived[pl.ds(part * 64, 64), :, lanes])
        product = table_times(table, which, jnp.concatenate([real, imag], axis=1))
        top, bottom = product[:HALF], product[HALF:]
        return top[:, :LANES] - bottom[:, LANES:], top[:, LANES:] + bottom[:, :LANES]

    def forward(part, which, value, lanes):
        product = table_times(table, which, value)
        top, bottom = product[:HALF], product[HALF:]
        sent[pl.ds(part * 64, 64), :, lanes] = merge_parts(
            top[:, :LANES] + bottom[:, LANES:], top[:, LANES:] - bottom[:, :LANES]
        )

    ranges = [pl.ds(start, LANES) for start in range(0, HALF, LANES)]
    waves = [(inverse(0, EVEN, lanes), inverse(1, ODD_T, lanes)) for lanes in ranges]
    for lanes, (even, odd) in zip(ranges, waves):
        damped = []
        for place, sign in enumerate((1.0, -1.0)):
            rows = pl.ds(place * HALF, HALF)
            real = even[0] + sign * odd[0]
            imag = even[1] + sign * odd[1]
            field[0, rows, lanes] = real
            field[1, rows, lanes] = imag
            absorb = damping[0, rows, lanes]
            phase = damping[1, rows, lanes]
            damped.append(
                jnp.concatenate([absorb * real - phase * imag, absorb * imag + phase * real], axis=1)
            )
        forward(0, EVEN, damped[0] + damped[1], lanes)
        forward(1, ODD, damped[0] - damped[1], lanes)


def on_cells(arrived, damping, table):
    shapes = (array(2, NY, HALF), array(DEVICES, 8, HALF))
    return call(cells_kernel, shapes, "cells", (), arrived, damping, table)


def product_of(real, signed_imag, value):
    return real * value + signed_imag * swapped(value)


def rotation(angle_tangent):
    side = signs((8, NX), -1.0, 1.0)
    inverse = 1.0 / (1.0 + angle_tangent * angle_tangent)
    return (
        (1.0 - angle_tangent * angle_tangent) * inverse,
        -2.0 * angle_tangent * inverse * side,
        inverse,
        -angle_tangent * inverse * side,
    )


def multiplied(left, right):
    return left[0] * right[0] - left[1] * right[1], left[0] * right[1] + left[1] * right[0]


PARTS = ((EVEN, EVEN, 1.0, pl.ds(0, HALF)), (ODD_T, ODD, -1.0, pl.ds(HALF, HALF)))


def rows_forward(block, count, table, into):
    pair = block.reshape(count, 2, 8, HALF)
    side = signs((1, 8, 1), 1.0, -1.0)
    for which, unused, sign, lanes in PARTS:
        value = pair[:, 0] + sign * pair[:, 1]
        value = jnp.concatenate([value, side * swapped(value)], axis=2).reshape(8 * count, NX)
        into[:, :, lanes] = times_table(value, table, which).reshape(count, 8, HALF)


def row_half(modes, table, which, lanes):
    side = signs((1, 8, 1), -1.0, 1.0)
    value = modes[:, :, lanes]
    value = jnp.concatenate([value, side * swapped(value)], axis=2).reshape(TIME * 8, NX)
    return times_table(value, table, which).reshape(TIME, 8, HALF)


def joined(even, odd, sent):
    sent[...] = jnp.stack([even + odd, even - odd], axis=1).reshape(DEVICES, 8, HALF)


def signed_power(turn, count):
    side = signs((8, NX), -1.0, 1.0)
    real, imag = turn[0], turn[1] * side
    for unused in range(count):
        real, imag = real * real - imag * imag, 2.0 * real * imag
    return real, imag, side


def closing(turn):
    real, imag, side = signed_power(turn, 6)
    real, imag = alpha * real, alpha * imag
    rest = 1.0 - real
    inverse = 1.0 / (rest * rest + imag * imag)
    return (real * rest - imag * imag) * inverse, (imag * rest + real * imag) * inverse * side


NORMAL = 1.0 / (NX * NY)


def columns_kernel(
    far_field, far_phase, far_absorb, trig, mine, theirs, field, phase, absorb, arrivals
):
    pairs = ((far_field, field), (far_phase, phase), (far_absorb, absorb))
    copies = [
        pltpu.make_async_copy(source, target, arrivals.at[place])
        for place, (source, target) in enumerate(pairs)
    ]
    for copy in copies:
        copy.start()
    trig_high, trig_low = halves(trig[...])

    def transformed(*values):
        high, low = halves(jnp.concatenate(values, axis=0))
        return dot_last(trig_high, high) + dot_last(trig_low, high) + dot_last(trig_high, low)

    copies[0].wait()
    real, imag = field[0], field[1]
    start_product = transformed(real, imag)
    copies[1].wait()
    copies[2].wait()
    damped_product = transformed(
        0.5 * (absorb[...] * real - phase[...] * imag),
        0.5 * (absorb[...] * imag + phase[...] * real),
    )
    upper = upper_rows((8, 1))
    for place, product in enumerate((start_product, damped_product)):
        first, second = product[:, :HALF], product[:, HALF:]
        real = first[:8] + second[8:]
        imag = second[:8] - first[8:]
        mine[place] = jnp.where(upper, real, swapped(imag))
        theirs[place] = jnp.where(upper, swapped(real), imag)


def columns_of(field, phase, absorb, trig):
    far = [pltpu.with_memory_space_constraint(value, pltpu.HBM) for value in (field, phase, absorb)]
    operands = (*far, trig)
    scratch = (
        pltpu.VMEM((2, HALF, NY), f32),
        pltpu.VMEM((HALF, NY), f32),
        pltpu.VMEM((HALF, NY), f32),
        pltpu.SemaphoreType.DMA((3,)),
    )
    shapes = (array(2, 8, HALF), array(2, 8, HALF))
    return call(columns_kernel, shapes, "columns", scratch, *operands, copied=3)


def turning_kernel(phase, absorb, damping):
    damping[0] = (0.5 / scale) * absorb[...].T
    damping[1] = (0.5 / scale) * phase[...].T


def turned(phase, absorb):
    return call(turning_kernel, array(2, NY, HALF), "turning", (), phase, absorb)


def tables_kernel(tangent, powers, ramps, closed):
    turn_real, turn_imag, gain_real, gain_imag = rotation(tangent[...])
    closed[0], closed[1] = closing((turn_real, turn_imag))
    power = jnp.ones((8, NX), f32), jnp.zeros((8, NX), f32)
    ramp = NORMAL * gain_real, NORMAL * gain_imag
    for n in range(TIME):
        for target, (real, imag) in ((powers, power), (ramps, ramp)):
            target[n, 0] = real
            target[n, 1] = imag
        power, ramp = [
            (real * turn_real - imag * turn_imag, real * turn_imag + imag * turn_real)
            for real, imag in (power, ramp)
        ]


def power_tables(tangent):
    shapes = (array(TIME, 2, 8, NX), array(TIME, 2, 8, NX), array(2, 8, NX))
    return call(tables_kernel, shapes, "tables", (), tangent)


def opening_kernel(block, tangent, table, powers, closed, vector, wrap_out, sent, spectrum, modes):
    rows_forward(block[...], 2, table, spectrum)
    slope = tangent[...]
    turn_real, turn_imag, gain_real, gain_imag = rotation(slope)
    side = signs((8, NX), -1.0, 1.0)
    wave, damped = spectrum[0], spectrum[1]
    vector[...] = product_of(1.0, -slope * side, wave) - damped
    value = product_of(turn_real, turn_imag, wave) - product_of(gain_real, gain_imag, damped)
    wrap = product_of(closed[0], closed[1], value)
    wrap_out[...] = product_of(1.0, slope * side, wrap)
    start = NORMAL * (wrap + value)
    found = []
    for part, (unused, which, sign, lanes) in enumerate(PARTS):
        here = start[:, part * HALF : (part + 1) * HALF]
        for n in range(TIME):
            modes[n, :, lanes] = product_of(powers[n, 0, :, lanes], powers[n, 1, :, lanes], here)
        found.append(row_half(modes, table, which, lanes))
    joined(*found, sent)


def opening(block, tangent, table, powers, closed):
    shapes = (array(8, NX), array(8, NX), array(DEVICES, 8, HALF))
    scratch = (pltpu.VMEM((2, 8, NX), f32), pltpu.VMEM((TIME, 8, NX), f32))
    operands = (block, tangent, table, powers, closed)
    return call(opening_kernel, shapes, "opening", scratch, *operands)


def modes_kernel_of(first):
    def body(
        block, table, powers, ramps, closed, earlier, wrap_in, vector, wrap_out, sent, modes, sums
    ):
        rows_forward(block[...], TIME, table, modes)
        start = (1.0 / scale) * wrap_in[...]
        if first:
            start = start - alpha * earlier[...]
        wraps = []
        for part in range(2):
            lanes = PARTS[part][3]
            before = start[:, part * HALF : (part + 1) * HALF]
            total = jnp.zeros((8, HALF), f32)
            for n in range(TIME):
                here = modes[n, :, lanes]
                value = here + before
                before = here
                if not first:
                    value = value - alpha * earlier[n, :, lanes]
                vector[n, :, lanes] = value
                real, imag = powers[n, 0, :, lanes], powers[n, 1, :, lanes]
                total = total + (real * value - imag * swapped(value))
                sums[n, :, lanes] = total
            wraps.append(product_of(closed[0, :, lanes], closed[1, :, lanes], total))
            wrap_out[:, lanes] = wraps[part]
        found = []
        for part, (unused, which, sign, lanes) in enumerate(PARTS):
            for n in range(TIME):
                modes[n, :, lanes] = product_of(
                    ramps[n, 0, :, lanes], ramps[n, 1, :, lanes], wraps[part] + sums[n, :, lanes]
                )
            found.append(row_half(modes, table, which, lanes))
        joined(*found, sent)

    return body


def on_modes(block, table, tables, earlier, wrap, first):
    shapes = (array(TIME, 8, NX), array(8, NX), array(DEVICES, 8, HALF))
    scratch = (pltpu.VMEM((TIME, 8, NX), f32), pltpu.VMEM((TIME, 8, NX), f32))
    body = modes_kernel_of(first)
    operands = (block, table, *tables, earlier, wrap)
    return call(body, shapes, "modes", scratch, *operands)


PAIRS = [(i, j) for i in range(1, ITERS + 1) for j in range(i, ITERS + 1)]


def products_kernel(block, table, w0, w1, w2, w3, wrap, totals, spectrum):
    rows_forward(block[...], TIME, table, spectrum)

    sums = [None] * (len(PAIRS) + ITERS + 1)
    order = [(0, j) for j in range(ITERS + 1)] + PAIRS

    def add(place, value):
        value = value[:, :LANES] + value[:, LANES:]
        sums[place] = value if sums[place] is None else sums[place] + value

    for part in range(2):
        lanes = PARTS[part][3]
        before = (1.0 / scale) * wrap[:, lanes]
        for n in range(TIME):
            here = spectrum[n, :, lanes]
            vectors = [w[n, :, lanes] for w in (w1, w2, w3)]
            vectors.append(here + before - alpha * vectors[2])
            vectors.insert(0, w0[:, lanes] if n == 0 else None)
            before = here
            for place, (i, j) in enumerate(order):
                if vectors[i] is not None:
                    add(place, vectors[i] * vectors[j])

    lane = lax.broadcasted_iota(jnp.int32, (1, 128), 1)
    packed = jnp.zeros((1, 128), f32)
    for place, total in enumerate(sums):
        total = jnp.sum(jnp.sum(total, axis=0, keepdims=True), axis=1, keepdims=True)
        packed = jnp.where(lane == place, total, packed)
    totals[...] = packed


def products(block, table, vectors, wrap):
    scratch = (pltpu.VMEM((TIME, 8, NX), f32),)
    operands = (block, table, *vectors, wrap)
    return call(products_kernel, array(1, 128), "products", scratch, *operands)


def least_squares(gram):
    size = ITERS + 1
    root = [[None] * size for unused in range(size)]
    for i in range(size):
        for j in range(i, size):
            total = gram[i][j]
            for k in range(i):
                total = total - root[k][i] * root[k][j]
            root[i][j] = jnp.sqrt(total) if i == j else total / root[i][i]
    matrix = [[jnp.zeros_like(gram[0][0]) for unused in range(ITERS)] for other in range(size)]
    for column in range(ITERS):
        for row in range(column + 2):
            total = scale * root[row][column + 1]
            if row <= column:
                total = total + (1.0 + shift) * root[row][column]
            matrix[row][column] = total
    target = [root[0][0]] + [jnp.zeros_like(gram[0][0]) for unused in range(ITERS)]
    cosines = []
    sines = []
    for column in range(ITERS):
        for row in range(column):
            upper = matrix[row][column]
            lower = matrix[row + 1][column]
            matrix[row][column] = cosines[row] * upper + sines[row] * lower
            matrix[row + 1][column] = -sines[row] * upper + cosines[row] * lower
        upper = matrix[column][column]
        lower = matrix[column + 1][column]
        radius = jnp.sqrt(upper * upper + lower * lower)
        cosines.append(upper / radius)
        sines.append(lower / radius)
        matrix[column][column] = radius
        target[column + 1] = -sines[column] * target[column]
        target[column] = cosines[column] * target[column]
    factors = [None] * ITERS
    for row in reversed(range(ITERS)):
        total = target[row]
        for other in range(row + 1, ITERS):
            total = total - matrix[row][other] * factors[other]
        factors[row] = total / matrix[row][row]
    return factors


def combine_kernel(totals, z0, z1, z2, z3, out):
    summed = jnp.sum(totals[...], axis=0, keepdims=True)
    size = ITERS + 1
    gram = [[None] * size for unused in range(size)]
    lane = lax.broadcasted_iota(jnp.int32, (1, 128), 1)
    order = [(0, j) for j in range(size)] + PAIRS
    for place, (i, j) in enumerate(order):
        value = jnp.sum(jnp.where(lane == place, summed, 0.0), axis=1, keepdims=True)
        gram[i][j] = value
        gram[j][i] = value
    factors = least_squares(gram)
    for part in range(2):
        value = factors[0] * z0[part]
        for factor, other in zip(factors[1:], (z1, z2, z3)):
            value = value + factor * other[part]
        out[part, 0] = value.T


def combine(totals, fields):
    return call(combine_kernel, array(2, 1, HALF, NY), "combine", (), totals, *fields)


def exchange(value):
    return lax.all_to_all(value, TM_SPACE, split_axis=0, concat_axis=0, tiled=True)


def column_modes(first, count):
    order = first + jnp.arange(count, dtype=jnp.int32)
    return 2 * (order % HALF) + order // HALF


def shards(u_init, phase, absorb):
    step = lax.axis_index(TM)
    half = lax.axis_index("space")
    table = jnp.asarray(TABLES)
    own = column_modes(4 * (2 * step + half), 4)
    other = column_modes(4 * (2 * (step ^ 2) + 1 - half), 4)
    turns = jnp.concatenate([own, other])[:, None] * jnp.arange(NY, dtype=jnp.int32)[None, :] % NY
    angle = turns.astype(f32) * (2.0 * math.pi / NY)
    trig = jnp.concatenate([jnp.cos(angle), jnp.sin(angle)])
    mine, theirs = columns_of(u_init, phase, absorb, trig)
    theirs = lax.ppermute(theirs, ("tm_2", "space"), [(0, 3), (1, 2), (2, 1), (3, 0)])
    block = jnp.where(
        half == 0, jnp.stack([mine, theirs], axis=1), jnp.stack([theirs, mine], axis=1)
    ).reshape(4, 8, HALF)
    own = own.astype(f32)
    rows = jnp.arange(HALF, dtype=jnp.int32)
    rows = jnp.concatenate([2 * rows, 2 * rows + 1]).astype(f32)
    symbol_y = 4.0 * jnp.sin(own * (math.pi / NY)) ** 2
    symbol_x = 4.0 * jnp.sin(rows * (math.pi / NX)) ** 2
    tangent = (0.5 * tau) * (jnp.concatenate([symbol_y, symbol_y])[:, None] + symbol_x[None, :])
    damping = turned(phase, absorb)
    tables = power_tables(tangent)
    block, damping, tables = lax.optimization_barrier((block, damping, tables))

    powers, ramps, closed = tables
    vector, wrap, sent = opening(block, tangent, table, powers, closed)
    vectors = [vector]
    found = []
    for column in range(ITERS):
        field, sent = on_cells(exchange(sent), damping, table)
        found.append(field)
        arrived = exchange(sent)
        if column + 1 < ITERS:
            vector, wrap, sent = on_modes(
                arrived, table, tables, vectors[-1], wrap, column == 0
            )
            vectors.append(vector)
    totals = products(arrived, table, vectors, wrap)
    return combine(exchange(jnp.broadcast_to(totals, (DEVICES, 128))), found)


def solution(mesh):
    torus = Mesh(
        mesh.devices.reshape(4, 4, 2, 2, mesh.shape["space"]),
        ("tm_0", "tm_1", "tm_2", "tm_3", "space"),
    )
    placed = (P(None, "space", None), P("space", None), P("space", None))
    return jax.shard_map(
        shards, mesh=torus, in_specs=placed, out_specs=P(None, TM, "space", None), check_vma=False
    )
```

```python
import math

import jax
import jax.numpy as jnp
import numpy as np
from jax import lax
from jax.experimental import pallas as pl
from jax.experimental.pallas import tpu as pltpu
from jax.sharding import Mesh
from jax.sharding import PartitionSpec as P

NX = 512
NY = 512
HALF = 256
LANES = 128
TIME = 64
ITERS = 4
DEVICES = 128
TM = ("tm_0", "tm_1", "tm_2", "tm_3")
TM_SPACE = ("tm_0", "tm_1", "tm_2", "tm_3", "space")

tau = 400.0
alpha = 0.4
shift = alpha * alpha / (1.0 - alpha * alpha)
scale = alpha / (1.0 - alpha * alpha)
f32 = jnp.float32
bf16 = jnp.bfloat16


def dft_tables():
    mode = np.arange(HALF)[:, None]
    cell = np.arange(HALF)[None, :]
    stack = []
    for frequency, transposed in ((2 * mode, False), (2 * mode + 1, False), (2 * mode + 1, True)):
        angle = 2.0 * np.pi * ((frequency * cell) % NX) / NX
        parts = [np.cos(angle), np.sin(angle)]
        stack.append(np.concatenate([part.T if transposed else part for part in parts]))
    exact = np.stack(stack)
    high = exact.astype(bf16)
    low = (exact - high.astype(np.float64)).astype(bf16)
    return np.stack([high, low])


TABLES = dft_tables()
EVEN, ODD, ODD_T = 0, 1, 2


def halves(value):
    high = value.astype(bf16)
    return high, (value - high.astype(f32)).astype(bf16)


def dot(left, right):
    return jnp.dot(left, right, preferred_element_type=f32)


def dot_last(left, right):
    return lax.dot_general(left, right, (((1,), (1,)), ((), ())), preferred_element_type=f32)


def table_times(table, which, value):
    high, low = halves(value)
    return dot(table[0, which], high) + dot(table[1, which], high) + dot(table[0, which], low)


def times_table(value, table, which):
    high, low = halves(value)
    return dot(high, table[0, which]) + dot(high, table[1, which]) + dot(low, table[0, which])


def call(body, out_shape, name, scratch, *operands, copied=0):
    inside = pl.BlockSpec(memory_space=pltpu.VMEM)
    return pl.pallas_call(
        body,
        out_shape=out_shape,
        in_specs=[pl.BlockSpec(memory_space=pltpu.HBM)] * copied + [inside] * (len(operands) - copied),
        out_specs=jax.tree.map(lambda unused: inside, out_shape),
        scratch_shapes=scratch,
        compiler_params=pltpu.CompilerParams(vmem_limit_bytes=24 << 20),
        name=name,
    )(*operands)


def array(*shape):
    return jax.ShapeDtypeStruct(shape, f32)


def upper_rows(shape):
    return lax.broadcasted_iota(jnp.int32, shape, len(shape) - 2) < 4


def swapped(value):
    return pltpu.roll(value, 4, value.ndim - 2)


def signs(shape, upper, lower):
    return jnp.where(upper_rows(shape), f32(upper), f32(lower))


def split_parts(block):
    pair = block.reshape(32, 2, 8, LANES)
    first, second = pair[:, 0], pair[:, 1]
    upper = upper_rows((1, 8, 1))
    real = jnp.where(upper, first, swapped(second))
    imag = jnp.where(upper, swapped(first), second)
    return real.reshape(HALF, LANES), imag.reshape(HALF, LANES)


def merge_parts(real, imag):
    real = real.reshape(32, 8, LANES)
    imag = imag.reshape(32, 8, LANES)
    upper = upper_rows((1, 8, 1))
    first = jnp.where(upper, real, swapped(imag))
    second = jnp.where(upper, swapped(real), imag)
    return jnp.stack([first, second], axis=1).reshape(64, 8, LANES)


def cells_kernel(arrived, damping, table, field, sent):
    def inverse(part, which, lanes):
        real, imag = split_parts(arrived[pl.ds(part * 64, 64), :, lanes])
        product = table_times(table, which, jnp.concatenate([real, imag], axis=1))
        top, bottom = product[:HALF], product[HALF:]
        return top[:, :LANES] - bottom[:, LANES:], top[:, LANES:] + bottom[:, :LANES]

    def forward(part, which, value, lanes):
        product = table_times(table, which, value)
        top, bottom = product[:HALF], product[HALF:]
        sent[pl.ds(part * 64, 64), :, lanes] = merge_parts(
            top[:, :LANES] + bottom[:, LANES:], top[:, LANES:] - bottom[:, :LANES]
        )

    ranges = [pl.ds(start, LANES) for start in range(0, HALF, LANES)]
    waves = [(inverse(0, EVEN, lanes), inverse(1, ODD_T, lanes)) for lanes in ranges]
    for lanes, (even, odd) in zip(ranges, waves):
        damped = []
        for place, sign in enumerate((1.0, -1.0)):
            rows = pl.ds(place * HALF, HALF)
            real = even[0] + sign * odd[0]
            imag = even[1] + sign * odd[1]
            field[0, rows, lanes] = real
            field[1, rows, lanes] = imag
            absorb = damping[0, rows, lanes]
            phase = damping[1, rows, lanes]
            damped.append(
                jnp.concatenate([absorb * real - phase * imag, absorb * imag + phase * real], axis=1)
            )
        forward(0, EVEN, damped[0] + damped[1], lanes)
        forward(1, ODD, damped[0] - damped[1], lanes)


def on_cells(arrived, damping, table):
    shapes = (array(2, NY, HALF), array(DEVICES, 8, HALF))
    return call(cells_kernel, shapes, "cells", (), arrived, damping, table)


def product_of(real, signed_imag, value):
    return real * value + signed_imag * swapped(value)


def rotation(angle_tangent):
    side = signs((8, NX), -1.0, 1.0)
    inverse = 1.0 / (1.0 + angle_tangent * angle_tangent)
    return (
        (1.0 - angle_tangent * angle_tangent) * inverse,
        -2.0 * angle_tangent * inverse * side,
        inverse,
        -angle_tangent * inverse * side,
    )


def multiplied(left, right):
    return left[0] * right[0] - left[1] * right[1], left[0] * right[1] + left[1] * right[0]


PARTS = ((EVEN, EVEN, 1.0, pl.ds(0, HALF)), (ODD_T, ODD, -1.0, pl.ds(HALF, HALF)))


def rows_forward(block, count, table, into):
    pair = block.reshape(count, 2, 8, HALF)
    side = signs((1, 8, 1), 1.0, -1.0)
    for which, unused, sign, lanes in PARTS:
        value = pair[:, 0] + sign * pair[:, 1]
        value = jnp.concatenate([value, side * swapped(value)], axis=2).reshape(8 * count, NX)
        into[:, :, lanes] = times_table(value, table, which).reshape(count, 8, HALF)


def row_half(modes, table, which, lanes):
    side = signs((1, 8, 1), -1.0, 1.0)
    value = modes[:, :, lanes]
    value = jnp.concatenate([value, side * swapped(value)], axis=2).reshape(TIME * 8, NX)
    return times_table(value, table, which).reshape(TIME, 8, HALF)


def joined(even, odd, sent):
    sent[...] = jnp.stack([even + odd, even - odd], axis=1).reshape(DEVICES, 8, HALF)


def signed_power(turn, count):
    side = signs((8, NX), -1.0, 1.0)
    real, imag = turn[0], turn[1] * side
    for unused in range(count):
        real, imag = real * real - imag * imag, 2.0 * real * imag
    return real, imag, side


def closing(turn):
    real, imag, side = signed_power(turn, 6)
    real, imag = alpha * real, alpha * imag
    rest = 1.0 - real
    inverse = 1.0 / (rest * rest + imag * imag)
    return (real * rest - imag * imag) * inverse, (imag * rest + real * imag) * inverse * side


NORMAL = 1.0 / (NX * NY)


def columns_kernel(
    far_field, far_phase, far_absorb, trig, mine, theirs, field, phase, absorb, arrivals
):
    pairs = ((far_field, field), (far_phase, phase), (far_absorb, absorb))
    copies = [
        pltpu.make_async_copy(source, target, arrivals.at[place])
        for place, (source, target) in enumerate(pairs)
    ]
    for copy in copies:
        copy.start()
    trig_high, trig_low = halves(trig[...])

    def transformed(*values):
        high, low = halves(jnp.concatenate(values, axis=0))
        return dot_last(trig_high, high) + dot_last(trig_low, high) + dot_last(trig_high, low)

    copies[0].wait()
    real, imag = field[0], field[1]
    start_product = transformed(real, imag)
    copies[1].wait()
    copies[2].wait()
    damped_product = transformed(
        0.5 * (absorb[...] * real - phase[...] * imag),
        0.5 * (absorb[...] * imag + phase[...] * real),
    )
    upper = upper_rows((8, 1))
    for place, product in enumerate((start_product, damped_product)):
        first, second = product[:, :HALF], product[:, HALF:]
        real = first[:8] + second[8:]
        imag = second[:8] - first[8:]
        mine[place] = jnp.where(upper, real, swapped(imag))
        theirs[place] = jnp.where(upper, swapped(real), imag)


def columns_of(field, phase, absorb, trig):
    far = [pltpu.with_memory_space_constraint(value, pltpu.HBM) for value in (field, phase, absorb)]
    operands = (*far, trig)
    scratch = (
        pltpu.VMEM((2, HALF, NY), f32),
        pltpu.VMEM((HALF, NY), f32),
        pltpu.VMEM((HALF, NY), f32),
        pltpu.SemaphoreType.DMA((3,)),
    )
    shapes = (array(2, 8, HALF), array(2, 8, HALF))
    return call(columns_kernel, shapes, "columns", scratch, *operands, copied=3)


def turning_kernel(phase, absorb, damping):
    damping[0] = (0.5 / scale) * absorb[...].T
    damping[1] = (0.5 / scale) * phase[...].T


def turned(phase, absorb):
    return call(turning_kernel, array(2, NY, HALF), "turning", (), phase, absorb)


def tables_kernel(tangent, powers, ramps, closed):
    turn_real, turn_imag, gain_real, gain_imag = rotation(tangent[...])
    closed[0], closed[1] = closing((turn_real, turn_imag))
    power = jnp.ones((8, NX), f32), jnp.zeros((8, NX), f32)
    ramp = NORMAL * gain_real, NORMAL * gain_imag
    for n in range(TIME):
        for target, (real, imag) in ((powers, power), (ramps, ramp)):
            target[n, 0] = real
            target[n, 1] = imag
        power, ramp = [
            (real * turn_real - imag * turn_imag, real * turn_imag + imag * turn_real)
            for real, imag in (power, ramp)
        ]


def power_tables(tangent):
    shapes = (array(TIME, 2, 8, NX), array(TIME, 2, 8, NX), array(2, 8, NX))
    return call(tables_kernel, shapes, "tables", (), tangent)


def opening_kernel(block, tangent, table, powers, closed, vector, wrap_out, sent, spectrum, modes):
    rows_forward(block[...], 2, table, spectrum)
    slope = tangent[...]
    turn_real, turn_imag, gain_real, gain_imag = rotation(slope)
    side = signs((8, NX), -1.0, 1.0)
    wave, damped = spectrum[0], spectrum[1]
    vector[...] = product_of(1.0, -slope * side, wave) - damped
    value = product_of(turn_real, turn_imag, wave) - product_of(gain_real, gain_imag, damped)
    wrap = product_of(closed[0], closed[1], value)
    wrap_out[...] = product_of(1.0, slope * side, wrap)
    start = NORMAL * (wrap + value)
    found = []
    for part, (unused, which, sign, lanes) in enumerate(PARTS):
        here = start[:, part * HALF : (part + 1) * HALF]
        for n in range(TIME):
            modes[n, :, lanes] = product_of(powers[n, 0, :, lanes], powers[n, 1, :, lanes], here)
        found.append(row_half(modes, table, which, lanes))
    joined(*found, sent)


def opening(block, tangent, table, powers, closed):
    shapes = (array(8, NX), array(8, NX), array(DEVICES, 8, HALF))
    scratch = (pltpu.VMEM((2, 8, NX), f32), pltpu.VMEM((TIME, 8, NX), f32))
    operands = (block, tangent, table, powers, closed)
    return call(opening_kernel, shapes, "opening", scratch, *operands)


def modes_kernel_of(first):
    def body(
        block, table, powers, ramps, closed, earlier, wrap_in, vector, wrap_out, sent, modes, sums
    ):
        rows_forward(block[...], TIME, table, modes)
        start = (1.0 / scale) * wrap_in[...]
        if first:
            start = start - alpha * earlier[...]
        wraps = []
        for part in range(2):
            lanes = PARTS[part][3]
            before = start[:, part * HALF : (part + 1) * HALF]
            total = jnp.zeros((8, HALF), f32)
            for n in range(TIME):
                here = modes[n, :, lanes]
                value = here + before
                before = here
                if not first:
                    value = value - alpha * earlier[n, :, lanes]
                vector[n, :, lanes] = value
                real, imag = powers[n, 0, :, lanes], powers[n, 1, :, lanes]
                total = total + (real * value - imag * swapped(value))
                sums[n, :, lanes] = total
            wraps.append(product_of(closed[0, :, lanes], closed[1, :, lanes], total))
            wrap_out[:, lanes] = wraps[part]
        found = []
        for part, (unused, which, sign, lanes) in enumerate(PARTS):
            for n in range(TIME):
                modes[n, :, lanes] = product_of(
                    ramps[n, 0, :, lanes], ramps[n, 1, :, lanes], wraps[part] + sums[n, :, lanes]
                )
            found.append(row_half(modes, table, which, lanes))
        joined(*found, sent)

    return body


def on_modes(block, table, tables, earlier, wrap, first):
    shapes = (array(TIME, 8, NX), array(8, NX), array(DEVICES, 8, HALF))
    scratch = (pltpu.VMEM((TIME, 8, NX), f32), pltpu.VMEM((TIME, 8, NX), f32))
    body = modes_kernel_of(first)
    operands = (block, table, *tables, earlier, wrap)
    return call(body, shapes, "modes", scratch, *operands)


PAIRS = [(i, j) for i in range(1, ITERS + 1) for j in range(i, ITERS + 1)]


def products_kernel(block, table, w0, w1, w2, w3, wrap, totals, spectrum):
    rows_forward(block[...], TIME, table, spectrum)

    sums = [None] * (len(PAIRS) + ITERS + 1)
    order = [(0, j) for j in range(ITERS + 1)] + PAIRS

    def add(place, value):
        value = value[:, :LANES] + value[:, LANES:]
        sums[place] = value if sums[place] is None else sums[place] + value

    for part in range(2):
        lanes = PARTS[part][3]
        before = (1.0 / scale) * wrap[:, lanes]
        for n in range(TIME):
            here = spectrum[n, :, lanes]
            vectors = [w[n, :, lanes] for w in (w1, w2, w3)]
            vectors.append(here + before - alpha * vectors[2])
            vectors.insert(0, w0[:, lanes] if n == 0 else None)
            before = here
            for place, (i, j) in enumerate(order):
                if vectors[i] is not None:
                    add(place, vectors[i] * vectors[j])

    lane = lax.broadcasted_iota(jnp.int32, (1, 128), 1)
    packed = jnp.zeros((1, 128), f32)
    for place, total in enumerate(sums):
        total = jnp.sum(jnp.sum(total, axis=0, keepdims=True), axis=1, keepdims=True)
        packed = jnp.where(lane == place, total, packed)
    totals[...] = packed


def products(block, table, vectors, wrap):
    scratch = (pltpu.VMEM((TIME, 8, NX), f32),)
    operands = (block, table, *vectors, wrap)
    return call(products_kernel, array(1, 128), "products", scratch, *operands)


def least_squares(gram):
    size = ITERS + 1
    root = [[None] * size for unused in range(size)]
    for i in range(size):
        for j in range(i, size):
            total = gram[i][j]
            for k in range(i):
                total = total - root[k][i] * root[k][j]
            root[i][j] = jnp.sqrt(total) if i == j else total / root[i][i]
    matrix = [[jnp.zeros_like(gram[0][0]) for unused in range(ITERS)] for other in range(size)]
    for column in range(ITERS):
        for row in range(column + 2):
            total = scale * root[row][column + 1]
            if row <= column:
                total = total + (1.0 + shift) * root[row][column]
            matrix[row][column] = total
    target = [root[0][0]] + [jnp.zeros_like(gram[0][0]) for unused in range(ITERS)]
    cosines = []
    sines = []
    for column in range(ITERS):
        for row in range(column):
            upper = matrix[row][column]
            lower = matrix[row + 1][column]
            matrix[row][column] = cosines[row] * upper + sines[row] * lower
            matrix[row + 1][column] = -sines[row] * upper + cosines[row] * lower
        upper = matrix[column][column]
        lower = matrix[column + 1][column]
        radius = jnp.sqrt(upper * upper + lower * lower)
        cosines.append(upper / radius)
        sines.append(lower / radius)
        matrix[column][column] = radius
        target[column + 1] = -sines[column] * target[column]
        target[column] = cosines[column] * target[column]
    factors = [None] * ITERS
    for row in reversed(range(ITERS)):
        total = target[row]
        for other in range(row + 1, ITERS):
            total = total - matrix[row][other] * factors[other]
        factors[row] = total / matrix[row][row]
    return factors


def combine_kernel(totals, z0, z1, z2, z3, out, result, departures):
    summed = jnp.sum(totals[...], axis=0, keepdims=True)
    size = ITERS + 1
    gram = [[None] * size for unused in range(size)]
    lane = lax.broadcasted_iota(jnp.int32, (1, 128), 1)
    order = [(0, j) for j in range(size)] + PAIRS
    for place, (i, j) in enumerate(order):
        value = jnp.sum(jnp.where(lane == place, summed, 0.0), axis=1, keepdims=True)
        gram[i][j] = value
        gram[j][i] = value
    factors = least_squares(gram)
    copies = []
    for part in range(2):
        for place in range(2):
            rows = pl.ds(place * LANES, LANES)
            value = factors[0] * z0[part, :, rows]
            for factor, other in zip(factors[1:], (z1, z2, z3)):
                value = value + factor * other[part, :, rows]
            result[part, rows] = value.T
            copy = pltpu.make_async_copy(
                result.at[part, rows], out.at[part, 0, rows], departures.at[2 * part + place]
            )
            copy.start()
            copies.append(copy)
    for copy in copies:
        copy.wait()


def combine(totals, fields):
    inside = pl.BlockSpec(memory_space=pltpu.VMEM)
    return pl.pallas_call(
        combine_kernel,
        out_shape=array(2, 1, HALF, NY),
        in_specs=[inside] * 5,
        out_specs=pl.BlockSpec(memory_space=pltpu.HBM),
        scratch_shapes=(pltpu.VMEM((2, HALF, NY), f32), pltpu.SemaphoreType.DMA((4,))),
        compiler_params=pltpu.CompilerParams(vmem_limit_bytes=24 << 20),
        name="combine",
    )(totals, *fields)


def exchange(value):
    return lax.all_to_all(value, TM_SPACE, split_axis=0, concat_axis=0, tiled=True)


def column_modes(first, count):
    order = first + jnp.arange(count, dtype=jnp.int32)
    return 2 * (order % HALF) + order // HALF


def shards(u_init, phase, absorb):
    step = lax.axis_index(TM)
    half = lax.axis_index("space")
    table = jnp.asarray(TABLES)
    own = column_modes(4 * (2 * step + half), 4)
    other = column_modes(4 * (2 * (step ^ 2) + 1 - half), 4)
    turns = jnp.concatenate([own, other])[:, None] * jnp.arange(NY, dtype=jnp.int32)[None, :] % NY
    angle = turns.astype(f32) * (2.0 * math.pi / NY)
    trig = jnp.concatenate([jnp.cos(angle), jnp.sin(angle)])
    mine, theirs = columns_of(u_init, phase, absorb, trig)
    theirs = lax.ppermute(theirs, ("tm_2", "space"), [(0, 3), (1, 2), (2, 1), (3, 0)])
    block = jnp.where(
        half == 0, jnp.stack([mine, theirs], axis=1), jnp.stack([theirs, mine], axis=1)
    ).reshape(4, 8, HALF)
    own = own.astype(f32)
    rows = jnp.arange(HALF, dtype=jnp.int32)
    rows = jnp.concatenate([2 * rows, 2 * rows + 1]).astype(f32)
    symbol_y = 4.0 * jnp.sin(own * (math.pi / NY)) ** 2
    symbol_x = 4.0 * jnp.sin(rows * (math.pi / NX)) ** 2
    tangent = (0.5 * tau) * (jnp.concatenate([symbol_y, symbol_y])[:, None] + symbol_x[None, :])
    damping = turned(phase, absorb)
    tables = power_tables(tangent)
    block, damping, tables = lax.optimization_barrier((block, damping, tables))

    powers, ramps, closed = tables
    vector, wrap, sent = opening(block, tangent, table, powers, closed)
    vectors = [vector]
    found = []
    for column in range(ITERS):
        field, sent = on_cells(exchange(sent), damping, table)
        found.append(field)
        arrived = exchange(sent)
        if column + 1 < ITERS:
            vector, wrap, sent = on_modes(
                arrived, table, tables, vectors[-1], wrap, column == 0
            )
            vectors.append(vector)
    totals = products(arrived, table, vectors, wrap)
    return combine(exchange(jnp.broadcast_to(totals, (DEVICES, 128))), found)


def solution(mesh):
    torus = Mesh(
        mesh.devices.reshape(4, 4, 2, 2, mesh.shape["space"]),
        ("tm_0", "tm_1", "tm_2", "tm_3", "space"),
    )
    placed = (P(None, "space", None), P("space", None), P("space", None))
    return jax.shard_map(
        shards, mesh=torus, in_specs=placed, out_specs=P(None, TM, "space", None), check_vma=False
    )
```
